512 devices in a mesh: energy: 64 (over x, y, z_lo), momentum: 2 (over core), phonon: 4 (over z_hi).
Axes of the slice: x: 4, y: 4, z: 16 (z_hi: 4, z_lo: 4; z = z_hi * 4 + z_lo), core: 2. Of those that a mesh axis runs over, the one named last changes fastest.
Arguments:
- g_less: bfloat16 [128, 2, 2, 144, 2176], P('energy', 'momentum', None, None, 'phonon'), may hold values from -6 to 6
- g_great: bfloat16 [128, 2, 2, 144, 2176], P('energy', 'momentum', None, None, 'phonon'), may hold values from -6 to 6
- d_less: float32 [1024, 2, 9, 17, 128], P(('energy', 'momentum', 'phonon')), may hold values from -0.5 to 0.5
- d_ret: bfloat16 [1024, 2, 384, 384], P(('energy', 'momentum', 'phonon')), may hold values from -0.21875 to 0.21875
- neighbours: int32 [17, 128], replicated, may hold values from 0 to 127
- bond_dirs: float32 [3, 17, 128], replicated, may hold values from -4 to 4
- energy_offset: int32 [1024], replicated, may hold values from 1 to 4
- momentum_offset: int32 [1024], replicated, may hold values from 0 to 1
- absorb: float32 [1024], replicated, may hold values from 0.1 to 0.9
Outputs:
- self_energy: bfloat16 [128, 2, 2, 144, 2176], P('energy', 'momentum', None, None, 'phonon')
- d_next: bfloat16 [1024, 2, 384, 384], P(('energy', 'momentum', 'phonon'))
The draws below stay inside these ranges and needn't reach their ends.
Inputs may be any that keep to these rules, and one draw needn't show every extreme that they name: `neighbours`: atoms of the window.
All inputs are finite; a program needn't handle non-finite values.
Results may differ from the reference program's by a relative error of at most 0.008.
Values may be sent and summed in bfloat16 or wider, within the bound.
A program may use at most 128 MiB of HBM per device.

```python
import math
import jax
import jax.numpy as jnp
from jax import lax

A = 128
NB = 17
ORB = 12
REACH = 4
NE = 128
NK = 2
MODES = 1024
ORDER = 384


def set_ends(result, stream_key, low, high):
    place = [jax.random.randint(jax.random.fold_in(stream_key, axis), (), 0, length) for axis, length in enumerate(result.shape)]
    widest = result.shape.index(max(result.shape))
    beside = place[:widest] + [(place[widest] + 1) % result.shape[widest]] + place[widest + 1:]
    return result.at[tuple(place)].set(low).at[tuple(beside)].set(high)


def shard_levels(rng, shape, cuts, low, largest):
    loudness = 1.0
    for dim, parts in cuts:
        steps = jax.random.uniform(jax.random.fold_in(jax.random.fold_in(rng, 6), dim), (parts,), jnp.float32, low / len(cuts), largest / len(cuts))
        loudness = loudness * jnp.repeat(jnp.exp(steps), shape[dim] // parts).reshape((-1,) + (1,) * (len(shape) - 1 - dim))
    return loudness


def gaussian(key, dims, deviation, most, cuts=(), held_as=jnp.bfloat16):
    loudness = shard_levels(key, dims, cuts, -0.22, 0.18) if cuts else 1.0
    values = jax.random.normal(key, dims, jnp.float32) * deviation * loudness
    return jnp.minimum(jnp.maximum(values, -most), most).astype(held_as)


def setup_inputs(seed: int = 0) -> dict:
    splits = jax.random.split(jax.random.key(seed), 10)
    return {
        "g_less": gaussian(splits[0], (NE, NK, 2, ORB * ORB, A * NB), 1.0, 6.0, ((0, 64), (1, 2), (4, 4))),
        "g_great": gaussian(splits[1], (NE, NK, 2, ORB * ORB, A * NB), 1.0, 6.0, ((0, 64), (1, 2), (4, 4))),
        "d_less": gaussian(splits[2], (MODES, 2, 9, NB, A), (MODES ** -0.5), 0.5, ((0, 512),), jnp.float32),
        "d_ret": gaussian(splits[3], (MODES, 2, ORDER, ORDER), (2 * ORDER) ** -0.5, 0.21875, ((0, 512),)),
        "neighbours": set_ends(jax.random.randint(splits[4], (NB, A), 0, A), jax.random.fold_in(splits[4], 1), 0, A - 1).astype(jnp.int32),
        "bond_dirs": gaussian(splits[5], (3, NB, A), 0.6, 4.0, (), jnp.float32),
        "energy_offset": set_ends(jax.random.randint(splits[6], (MODES,), 1, REACH + 1), jax.random.fold_in(splits[6], 1), 1, REACH).astype(jnp.int32),
        "momentum_offset": set_ends(jax.random.randint(splits[7], (MODES,), 0, NK), jax.random.fold_in(splits[7], 1), 0, NK - 1).astype(jnp.int32),
        "absorb": jnp.clip(jnp.exp(jax.random.uniform(splits[8], (MODES,), jnp.float32, math.log(0.1), math.log(0.9))), 0.1, 0.9),
    }


HIGH = lax.Precision.HIGHEST


def complex_scale(weight, block):
    real_w = weight[0]
    imag_w = weight[1]
    real_b = block[:, :, 0].astype(jnp.float32)
    imag_b = block[:, :, 1].astype(jnp.float32)
    return jnp.stack([real_w * real_b - imag_w * imag_b, real_w * imag_b + imag_w * real_b], axis=2)


def reference(g_less, g_great, d_less, d_ret, neighbours, bond_dirs, energy_offset, momentum_offset, absorb):
    classes = REACH * NK
    entries = ORB * ORB
    pair_cube = bond_dirs[:, None] * bond_dirs[None, :]
    pair = pair_cube.reshape(9, NB, A)
    coupling = jnp.sum(d_less * pair[None, None], axis=2)
    label = (energy_offset - 1) * NK + momentum_offset
    table = (label[:, None] == jnp.arange(classes, dtype=jnp.int32)[None, :]).astype(jnp.float32)
    flat = coupling.reshape(MODES, -1)
    emitted = jnp.dot(table.T, flat, precision=HIGH).reshape(classes, 2, NB, A).transpose(3, 0, 1, 2)
    absorbed = jnp.dot((table * absorb[:, None]).T, flat, precision=HIGH).reshape(classes, 2, NB, A).transpose(3, 0, 1, 2)
    lesser = g_less.reshape(NE, NK, 2, entries, A, NB).transpose(4, 0, 1, 2, 3, 5)
    greater = g_great.reshape(NE, NK, 2, entries, A, NB).transpose(4, 0, 1, 2, 3, 5)
    scale = float(NE * NK * ORB * ORB) ** -0.5
    zero_pad = ((0, 0), (0, 0), (0, 0), (0, 0))

    def per_atom(items):
        low_blocks, high_blocks, emit_atom, soak_atom = items
        low_padded = jnp.pad(low_blocks, ((REACH, REACH),) + zero_pad)
        high_padded = jnp.pad(high_blocks, ((REACH, 0),) + zero_pad)
        total = jnp.zeros(low_blocks.shape, jnp.float32)
        low_real = low_blocks[:, :, 0].astype(jnp.float32)
        low_imag = low_blocks[:, :, 1].astype(jnp.float32)
        polar_list = []
        for energy_step in range(1, REACH + 1):
            for moment_step in range(NK):
                index = (energy_step - 1) * NK + moment_step
                below = jnp.roll(low_padded[REACH - energy_step: REACH - energy_step + NE], moment_step, axis=1)
                above = jnp.roll(low_padded[REACH + energy_step: REACH + energy_step + NE], -moment_step, axis=1)
                total = total + complex_scale(emit_atom[index], below) + complex_scale(soak_atom[index], above)
                earlier = jnp.roll(high_padded[REACH - energy_step: REACH - energy_step + NE], moment_step, axis=1)
                high_real = earlier[:, :, 0].astype(jnp.float32)
                high_imag = earlier[:, :, 1].astype(jnp.float32)
                real_sum = jnp.sum(low_real * high_real + low_imag * high_imag, axis=(0, 1, 2))
                imag_sum = jnp.sum(low_imag * high_real - low_real * high_imag, axis=(0, 1, 2))
                polar_list.append(jnp.stack([real_sum, imag_sum], axis=1) * scale)
        return total.astype(jnp.bfloat16), jnp.stack(polar_list)

    sigma_atoms, polar_atoms = lax.map(per_atom, (lesser, greater, emitted, absorbed))
    self_energy = sigma_atoms.transpose(1, 2, 3, 4, 0, 5).reshape(NE, NK, 2, entries, A * NB)
    polar_modes = jnp.einsum('mc,acnz->manz', table, polar_atoms, precision=HIGH)
    link = (neighbours[:, :, None] == jnp.arange(A, dtype=jnp.int32)[None, None, :]).astype(jnp.float32)

    def per_mode(items):
        polar_one, ret_one = items
        dense_list = []
        for part in range(2):
            weighted = pair_cube * polar_one[:, :, part].T[None, None]
            dense = jnp.einsum('ijna,nab->iajb', weighted, link, precision=HIGH).reshape(ORDER, ORDER)
            dense_list.append(dense.astype(jnp.bfloat16))
        dense_re, dense_im = dense_list
        ret_re, ret_im = ret_one[0], ret_one[1]
        half_re = (jnp.dot(dense_re, ret_re.T, preferred_element_type=jnp.float32)
                   + jnp.dot(dense_im, ret_im.T, preferred_element_type=jnp.float32)).astype(jnp.bfloat16)
        half_im = (jnp.dot(dense_im, ret_re.T, preferred_element_type=jnp.float32)
                   - jnp.dot(dense_re, ret_im.T, preferred_element_type=jnp.float32)).astype(jnp.bfloat16)
        next_re = jnp.dot(ret_re, half_re, preferred_element_type=jnp.float32) - jnp.dot(ret_im, half_im, preferred_element_type=jnp.float32)
        next_im = jnp.dot(ret_re, half_im, preferred_element_type=jnp.float32) + jnp.dot(ret_im, half_re, preferred_element_type=jnp.float32)
        return jnp.stack([next_re, next_im]).astype(jnp.bfloat16)

    d_next = lax.map(per_mode, (polar_modes, d_ret))
    return self_energy, d_next
```

```python
import functools

import jax
import jax.numpy as jnp
from jax import lax
from jax.experimental import pallas as pl
from jax.experimental.pallas import tpu as pltpu
from jax.sharding import Mesh
from jax.sharding import PartitionSpec as P

ORB = 12
REACH = 4
X, Y, Z, C, H = ("energy_0", "energy_1", "energy_2", "momentum", "phonon")
ENERGY = (X, Y, Z)
HIGH = lax.Precision.HIGHEST
MESH = pl.DeviceIdType.MESH
ROWS = 160
BF = jnp.bfloat16
F32 = jnp.float32
DMA = pltpu.SemaphoreType.DMA


def others(axis, size):
    here = lax.axis_index(axis)
    return [lax.rem(here + d, size) for d in range(1, size)]


def greet(barrier, **target):
    pl.semaphore_signal(barrier, inc=1, device_id=target, device_id_type=MESH)


def remote(src, dst, send, recv, target):
    return pltpu.make_async_remote_copy(
        src_ref=src, dst_ref=dst, send_sem=send, recv_sem=recv,
        device_id=target, device_id_type=MESH,
    )


def swap(src, dst, send, recv, axis, size):
    here = lax.axis_index(axis)
    copies = []
    for d in range(1, size):
        copies.append(
            remote(src, dst.at[d - 1], send.at[d - 1], recv.at[d - 1],
                   {axis: lax.rem(here + d, size)})
        )
    for c in copies:
        c.start()
    return copies


def gather_kernel(
    gl, gg, rl, rg, dl, bd, eo, mo, ab,
    gl_out, gg_out, w_out,
    GL, GG, CP, YB, YR, T, TC, T0, T1, T2, TY, TX, TZ, WF,
    zs_send, zs_recv, gs_send, gs_recv, row_send, row_recv, part_send, part_recv,
    y_send, y_recv, ts_send, ts_recv, ty_send, ty_recv, tx_send, tx_recv, tz_send, tz_recv,
    ta_send, ta_recv, out_sem,
):
    x, y, z, c, h = (lax.axis_index(n) for n in (X, Y, Z, C, H))
    row = x * 4 + y
    mate = {C: 1 - c}

    barrier = pltpu.get_barrier_semaphore()
    greet(barrier, **mate)
    for axis, size in ((Z, 4), (Y, 4), (X, 4), (H, 4)):
        for o in others(axis, size):
            greet(barrier, **{axis: o})
    crosses_up = jnp.logical_and(y == 3, x < 3)
    crosses_down = jnp.logical_and(y == 0, x > 0)

    @pl.when(crosses_up)
    def _():
        greet(barrier, **{X: x + 1, Y: 0})

    @pl.when(crosses_down)
    def _():
        greet(barrier, **{X: x - 1, Y: 3})

    def own(src, extra, dst, block, sem):
        return [
            pltpu.make_async_copy(
                src.at[:, 0, :, :, pl.ds(pl.multiple_of(z * 128, 128), 128)],
                dst.at[block, :, :, pl.ds(0, 144), :], sem.at[z, 0]),
            pltpu.make_async_copy(
                extra.at[z], dst.at[block, :, :, pl.ds(144, 16), :], sem.at[z, 1]),
        ]

    for cp in own(gl, rl, GL.at[0], 2 + z, zs_recv) + own(gg, rg, GG, z, gs_recv):
        cp.start()

    lane = lax.broadcasted_iota(jnp.int32, (24, 128), 1)
    CP[...] = jnp.zeros_like(CP)
    for m in range(2):
        for part in range(2):
            total = None
            for i in range(3):
                for j in range(3):
                    term = dl[m, part, 3 * i + j] * (bd[i] * bd[j])
                    total = term if total is None else total + term
            CP[2 * m + part, pl.ds(0, 17), :] = total
    for p in range(4):
        grouped = jnp.zeros((24, 128), F32)
        for k in range(4):
            shift = ((k - p) * 32) % 128
            piece = CP[k]
            if shift:
                piece = pltpu.roll(piece, shift, 1)
            grouped = jnp.where((lane >> 5) == k, piece, grouped)
        YB[p] = grouped
    YR[3] = YB[h]

    @pl.when(row == 0)
    def _():
        GL[:, pl.ds(0, 2)] = jnp.zeros((2, 2, 2, 2, ROWS, 128), BF)

    @pl.when(row == 15)
    def _():
        GL[:, pl.ds(6, 2)] = jnp.zeros((2, 2, 2, 2, ROWS, 128), BF)

    extra = jnp.where(crosses_up, 1, 0) + jnp.where(crosses_down, 1, 0)
    pl.semaphore_wait(barrier, 13 + extra)

    y_copies = []
    for d in range(1, 4):
        to = lax.rem(h + d, 4)
        y_copies.append(
            remote(YB.at[to], YR.at[d - 1], y_send.at[d - 1], y_recv.at[d - 1], {H: to})
        )
    for cp in y_copies:
        cp.start()

    def tiles(src, extra, dst, block, send, recv, p):
        return [
            remote(src.at[:, 0, :, :, pl.ds(pl.multiple_of(p * 128, 128), 128)],
                   dst.at[block, :, :, pl.ds(0, 144), :], send.at[p, 0], recv.at[z, 0], {Z: p}),
            remote(extra.at[p], dst.at[block, :, :, pl.ds(144, 16), :],
                   send.at[p, 1], recv.at[z, 1], {Z: p}),
        ]

    def less_tiles(p):
        return tiles(gl, rl, GL.at[0], 2 + z, zs_send, zs_recv, p)

    def great_tiles(p):
        return tiles(gg, rg, GG, z, gs_send, gs_recv, p)

    for make in (less_tiles, great_tiles):
        for j in range(4):
            p = jnp.where(z < 2, 3 - j, j)

            @pl.when(p != z)
            def _(make=make, p=p):
                for cp in make(p):
                    cp.start()

    def arrived(dst, block, recv, s):
        for k, (a, n) in enumerate(((0, 144), (144, 16))):
            ref = dst.at[block, :, :, pl.ds(a, n), :]
            pltpu.make_async_copy(ref, ref, recv.at[s, k]).wait()

    def to_mate(b):
        return remote(GL.at[0, b], GL.at[1, b], part_send.at[b], part_recv.at[b], mate)

    def next_row(s):
        up = row + 1
        return remote(GL.at[0, 2 + s], GL.at[0, s - 2], row_send.at[s], row_recv.at[s],
                      {X: up // 4, Y: lax.rem(up, 4)})

    def last_row(s):
        down = row - 1
        return remote(GL.at[0, 2 + s], GL.at[0, s + 6], row_send.at[s], row_recv.at[s],
                      {X: down // 4, Y: lax.rem(down, 4)})

    def forward(s):
        arrived(GL.at[0], 2 + s, zs_recv, s)

        @pl.when(jnp.logical_and(s >= 2, row < 15))
        def _():
            next_row(s).start()

        @pl.when(jnp.logical_and(s < 2, row > 0))
        def _():
            last_row(s).start()

        to_mate(2 + s).start()

    forward(z)

    for cp in y_copies:
        cp.wait_recv()
    lane64 = lane < 64
    base = ((((row * 4 + z) * 2 + c) * 4) * 2)
    label, soak = [], []
    for d in range(4):
        from_h = lax.rem(h + 4 - (d + 1), 4)
        for m in range(2):
            g = base + from_h * 2 + m
            label.append((eo[g] - 1) * 2 + mo[g])
            soak.append(ab[g])
    for q in range(2):
        for e in range(4):
            emit = jnp.zeros((24, 128), F32)
            taken = jnp.zeros((24, 128), F32)
            for d in range(4):
                v = YR[d]
                on = [jnp.where(label[2 * d + m] == 2 * e + q, 1.0, 0.0).astype(F32) for m in range(2)]
                on_s = [on[m] * soak[2 * d + m] for m in range(2)]
                emit = emit + v * jnp.where(lane64, on[0], on[1])
                taken = taken + v * jnp.where(lane64, on_s[0], on_s[1])
            emit = emit + pltpu.roll(emit, 64, 1)
            taken = taken + pltpu.roll(taken, 64, 1)
            T[q, e] = jnp.where(lane64, emit, taken)
    ts = remote(T.at[1 - c], TC, ts_send, ts_recv, mate)
    ts.start()

    forward(lax.rem(z + 1, 4))
    ts.wait_recv()
    T0[...] = T[c] + TC[...]
    ty = swap(T0, TY, ty_send, ty_recv, Y, 4)
    forward(lax.rem(z + 3, 4))
    for cp in ty:
        cp.wait_recv()
    T1[...] = (T0[...] + TY[0]) + (TY[1] + TY[2])
    tx = swap(T1, TX, tx_send, tx_recv, X, 4)
    forward(lax.rem(z + 2, 4))
    for cp in tx:
        cp.wait_recv()
    T2[...] = (T1[...] + TX[0]) + (TX[1] + TX[2])
    tz = swap(T2, TZ, tz_send, tz_recv, Z, 4)

    @pl.when(row > 0)
    def _():
        for b in (0, 1):
            ref = GL.at[0, b]
            pltpu.make_async_copy(ref, ref, row_recv.at[b + 2]).wait()
            to_mate(b).start()

    @pl.when(row < 15)
    def _():
        for b in (6, 7):
            ref = GL.at[0, b]
            pltpu.make_async_copy(ref, ref, row_recv.at[b - 6]).wait()
            to_mate(b).start()

    for cp in tz:
        cp.wait_recv()
    WF[c] = (T2[...] + TZ[0]) + (TZ[1] + TZ[2])
    ta = remote(WF.at[c], WF.at[c], ta_send, ta_recv, mate)
    ta.start()

    def from_mate(b):
        ref = GL.at[1, b]
        pltpu.make_async_copy(ref, ref, part_recv.at[b]).wait()

    for b in range(2, 6):
        from_mate(b)

    @pl.when(row > 0)
    def _():
        from_mate(0)
        from_mate(1)

    @pl.when(row < 15)
    def _():
        from_mate(6)
        from_mate(7)

    less_out = pltpu.make_async_copy(GL, gl_out, out_sem.at[0])
    less_out.start()
    ta.wait_recv()
    w_out[...] = WF[...]
    for s in range(4):
        arrived(GG, s, gs_recv, s)
    great_out = pltpu.make_async_copy(GG, gg_out, out_sem.at[1])
    great_out.start()

    for cp in y_copies + ty + tx + tz + [ts, ta]:
        cp.wait_send()
    for s in range(4):
        @pl.when(z != s)
        def _(s=s):
            for cp in less_tiles(s) + great_tiles(s):
                cp.wait_send()

        to_mate(2 + s).wait_send()

    @pl.when(row < 15)
    def _():
        for s in (2, 3):
            next_row(s).wait_send()
        for b in (6, 7):
            to_mate(b).wait_send()

    @pl.when(row > 0)
    def _():
        for s in (0, 1):
            last_row(s).wait_send()
        for b in (0, 1):
            to_mate(b).wait_send()

    less_out.wait()
    great_out.wait()


def gather(gl, gg, rl, rg, dl, bd, eo, mo, ab):
    anyspace = pl.BlockSpec(memory_space=pl.ANY)
    vmem = pl.BlockSpec(memory_space=pltpu.VMEM)
    smem = pl.BlockSpec(memory_space=pltpu.SMEM)
    t = (4, 24, 128)
    return pl.pallas_call(
        gather_kernel,
        out_shape=(
            jax.ShapeDtypeStruct((2, 8, 2, 2, ROWS, 128), BF),
            jax.ShapeDtypeStruct((4, 2, 2, ROWS, 128), BF),
            jax.ShapeDtypeStruct((2,) + t, F32),
        ),
        in_specs=[anyspace] * 4 + [vmem] * 2 + [smem] * 3,
        out_specs=(anyspace, anyspace, vmem),
        scratch_shapes=[
            pltpu.VMEM((2, 8, 2, 2, ROWS, 128), BF),
            pltpu.VMEM((4, 2, 2, ROWS, 128), BF),
            pltpu.VMEM(t, F32), pltpu.VMEM(t, F32), pltpu.VMEM(t, F32),
            pltpu.VMEM((2,) + t, F32), pltpu.VMEM(t, F32),
            pltpu.VMEM(t, F32), pltpu.VMEM(t, F32), pltpu.VMEM(t, F32),
            pltpu.VMEM((3,) + t, F32), pltpu.VMEM((3,) + t, F32), pltpu.VMEM((3,) + t, F32),
            pltpu.VMEM((2,) + t, F32),
            DMA((4, 2)), DMA((4, 2)), DMA((4, 2)), DMA((4, 2)), DMA((4,)), DMA((4,)),
            DMA((8,)), DMA((8,)), DMA((3,)), DMA((3,)), DMA, DMA,
            DMA((3,)), DMA((3,)), DMA((3,)), DMA((3,)), DMA((3,)), DMA((3,)), DMA, DMA, DMA((2,)),
        ],
        compiler_params=pltpu.CompilerParams(
            collective_id=1, has_side_effects=True, vmem_limit_bytes=40 << 20
        ),
        name="gather_blocks",
    )(gl, gg, rl, rg, dl, bd, eo, mo, ab)


def blocks_kernel(
    scale, gl, gg, w, s_out, r_out, p_out,
    SB, WB, PA, PS, PC, P0, P1, P2, PY, PX, PG,
    s_send, s_recv, c_send, c_recv, y_send, y_recv, x_send, x_recv, z_send, z_recv,
    a_send, a_recv,
):
    x, y, z, c, h = (lax.axis_index(n) for n in (X, Y, Z, C, H))
    mate = {C: 1 - c}
    zz = h * 4 + z
    barrier = pltpu.get_barrier_semaphore()
    greet(barrier, **mate)
    for axis, size in ((Y, 4), (X, 4)):
        for o in others(axis, size):
            greet(barrier, **{axis: o})
    for d in range(1, 16):
        o = lax.rem(zz + d, 16)
        greet(barrier, **{Z: lax.rem(o, 4), H: o // 4})

    PA[...] = jnp.zeros_like(PA)

    def polar_rows(i, carry):
        rows = pl.ds(pl.multiple_of(i * 16, 16), 16)
        acc = [jnp.zeros((8, 128), F32) for _ in range(16)]
        for energy in range(8):
            hr = gg[energy, 0, rows, :].astype(F32)
            hi = gg[energy, 1, rows, :].astype(F32)
            for q in range(2):
                for e in range(4):
                    lr = gl[q, 5 + energy + e, 0, rows, :].astype(F32)
                    li = gl[q, 5 + energy + e, 1, rows, :].astype(F32)
                    re = lr * hr + li * hi
                    im = li * hr - lr * hi
                    k = q * 8 + e * 2
                    acc[k] = acc[k] + (re[:8] + re[8:])
                    acc[k + 1] = acc[k + 1] + (im[:8] + im[8:])
        last = i // 9
        for k in range(16):
            PA[last, k] += acc[k]
        return carry

    lax.fori_loop(0, 10, polar_rows, 0)
    for q in range(2):
        for last in range(2):
            for k in range(8):
                PS[q, pl.ds(last * 8 + k, 1), :] = (
                    jnp.sum(PA[last, q * 8 + k], axis=0, keepdims=True) * scale
                )
    pl.semaphore_wait(barrier, 22)
    pc = remote(PS.at[1 - c], PC, c_send, c_recv, mate)
    pc.start()

    col = lax.broadcasted_iota(jnp.int32, (128, 256), 1)
    col = jnp.where(col < 128, z * 128 + col, 512 + (col & 31))
    src = lax.broadcasted_iota(jnp.int32, (128, 256), 0)
    off = col - 17 * (src & 31)
    inside = jnp.logical_and(off >= 0, off < 17)
    col24 = lax.broadcasted_iota(jnp.int32, (24, 256), 1)
    col24 = jnp.where(col24 < 128, z * 128 + col24, 512 + (col24 & 31))
    atom = jnp.floor((col24.astype(F32) + 0.5) * (1.0 / 17.0))
    bond = col24.astype(F32) - 17.0 * atom
    pick = bond == lax.broadcasted_iota(jnp.int32, (24, 256), 0).astype(F32)
    flat = w[...].reshape(192, 128)
    for k in range(4):
        e_k = jnp.where(jnp.logical_and(inside, (src >> 5) == k), 1.0, 0.0).astype(F32)
        spread = jnp.dot(flat, e_k, precision=HIGH, preferred_element_type=F32)
        for qe in range(8):
            line = jnp.sum(jnp.where(pick, spread[qe * 24:(qe + 1) * 24], 0.0), axis=0, keepdims=True)
            WB[0, qe * 4 + k] = jnp.broadcast_to(line[:, :128], (8, 128))
            WB[1, qe * 4 + k] = jnp.broadcast_to(line[:, 128:], (8, 128))

    def sigma_rows(i, carry):
        rows = pl.ds(pl.multiple_of(i * 16, 16), 16)
        last = i // 9
        for energy in range(8):
            re = jnp.zeros((2, 8, 128), F32)
            im = jnp.zeros((2, 8, 128), F32)
            for q in range(2):
                for e in range(4):
                    for k, at in ((0, 3 + energy - e), (2, 5 + energy + e)):
                        br = gl[q, at, 0, rows, :].astype(F32).reshape(2, 8, 128)
                        bi = gl[q, at, 1, rows, :].astype(F32).reshape(2, 8, 128)
                        wr = WB[last, (q * 4 + e) * 4 + k][None]
                        wi = WB[last, (q * 4 + e) * 4 + k + 1][None]
                        re = re + (wr * br - wi * bi)
                        im = im + (wr * bi + wi * br)
            SB[energy, 0, rows, :] = re.reshape(16, 128).astype(BF)
            SB[energy, 1, rows, :] = im.reshape(16, 128).astype(BF)
        return carry

    pc.wait_recv()
    P0[...] = PS[c] + PC[...]
    py = swap(P0, PY, y_send, y_recv, Y, 4)
    lax.fori_loop(0, 5, sigma_rows, 0)
    for cp in py:
        cp.wait_recv()
    P1[...] = (P0[...] + PY[0]) + (PY[1] + PY[2])
    px = swap(P1, PX, x_send, x_recv, X, 4)
    lax.fori_loop(5, 10, sigma_rows, 0)
    for cp in px:
        cp.wait_recv()
    PG[c, zz] = (P1[...] + PX[0]) + (PX[1] + PX[2])
    P2[...] = (P1[...] + PX[0]) + (PX[1] + PX[2])
    pz = []
    for d in range(1, 16):
        o = lax.rem(zz + d, 16)
        pz.append(
            remote(P2, PG.at[c, zz], z_send.at[d - 1], z_recv.at[d - 1],
                   {Z: lax.rem(o, 4), H: o // 4})
        )
    for d in (8, 7, 9, 6, 10, 5, 11, 4, 12, 3, 13, 2, 14, 1, 15):
        pz[d - 1].start()

    def back(p):
        return [
            remote(SB.at[pl.ds(2 * p, 2), :, pl.ds(0, 144), :],
                   s_out.at[:, :, :, pl.ds(pl.multiple_of(z * 128, 128), 128)],
                   s_send.at[p, 0], s_recv.at[z, 0], {Z: p}),
            remote(SB.at[pl.ds(2 * p, 2), :, pl.ds(144, 16), :], r_out.at[z],
                   s_send.at[p, 1], s_recv.at[z, 1], {Z: p}),
        ]

    for j in range(4):
        p = jnp.where(z < 2, 3 - j, j)

        @pl.when(p != z)
        def _(p=p):
            for cp in back(p):
                cp.start()

    pltpu.make_async_copy(
        SB.at[pl.ds(2 * z, 2), :, pl.ds(0, 144), :],
        s_out.at[:, :, :, pl.ds(pl.multiple_of(z * 128, 128), 128)], s_recv.at[z, 0]).start()
    pltpu.make_async_copy(
        SB.at[pl.ds(2 * z, 2), :, pl.ds(144, 16), :], r_out.at[z], s_recv.at[z, 1]).start()

    for d in range(1, 16):
        o = lax.rem(zz + 16 - d, 16)
        ref = PG.at[c, o]
        pltpu.make_async_copy(ref, ref, z_recv.at[d - 1]).wait()
    pa = remote(PG.at[c], PG.at[c], a_send, a_recv, mate)
    pa.start()
    pa.wait_recv()
    p_out[...] = PG[...]

    for s in range(4):
        main = s_out.at[:, :, :, pl.ds(s * 128, 128)]
        pltpu.make_async_copy(main, main, s_recv.at[s, 0]).wait()
        pltpu.make_async_copy(r_out.at[s], r_out.at[s], s_recv.at[s, 1]).wait()

        @pl.when(z != s)
        def _(s=s):
            for cp in back(s):
                cp.wait_send()
    for cp in [pc, pa] + py + px + pz:
        cp.wait_send()


def blocks(scale, gl, gg, w):
    anyspace = pl.BlockSpec(memory_space=pl.ANY)
    vmem = pl.BlockSpec(memory_space=pltpu.VMEM)
    p = (16, 128)
    return pl.pallas_call(
        functools.partial(blocks_kernel, scale),
        out_shape=(
            jax.ShapeDtypeStruct((2, 2, 144, 512), BF),
            jax.ShapeDtypeStruct((4, 2, 2, 16, 128), BF),
            jax.ShapeDtypeStruct((2, 16) + p, F32),
        ),
        in_specs=[vmem] * 3,
        out_specs=(anyspace, anyspace, vmem),
        scratch_shapes=[
            pltpu.VMEM((8, 2, ROWS, 128), BF),
            pltpu.VMEM((2, 32, 8, 128), F32),
            pltpu.VMEM((2, 16, 8, 128), F32),
            pltpu.VMEM((2,) + p, F32),
            pltpu.VMEM(p, F32), pltpu.VMEM(p, F32), pltpu.VMEM(p, F32), pltpu.VMEM(p, F32),
            pltpu.VMEM((3,) + p, F32), pltpu.VMEM((3,) + p, F32),
            pltpu.VMEM((2, 16) + p, F32),
            DMA((4, 2)), DMA((4, 2)), DMA, DMA, DMA((3,)), DMA((3,)), DMA((3,)), DMA((3,)),
            DMA((15,)), DMA((15,)), DMA, DMA,
        ],
        compiler_params=pltpu.CompilerParams(
            collective_id=2, has_side_effects=True, vmem_limit_bytes=40 << 20
        ),
        name="self_energy_and_polar",
    )(gl, gg, w)


def phonon_kernel(pg, bd, nb, eo, mo, ret, out, D, L, N, W, DT, HT):
    x, y, z, c, h = (lax.axis_index(n) for n in (X, Y, Z, C, H))
    base = ((((x * 4 + y) * 4 + z) * 2 + c) * 4 + h) * 2
    for m in range(2):
        e = eo[base + m] - 1
        q = mo[base + m]
        for part in range(2):
            for o in range(16):
                for last in range(2):
                    D[last, 2 * m + part, pl.ds(o, 1), :] = pg[
                        q, o, pl.ds(last * 8 + e * 2 + part, 1), :]
    lane = lax.broadcasted_iota(jnp.int32, (24, 128), 1)
    sub = lax.broadcasted_iota(jnp.int32, (24, 128), 0)
    lane128 = lax.broadcasted_iota(jnp.int32, (128, 128), 1)
    sub128 = lax.broadcasted_iota(jnp.int32, (128, 128), 0)
    total = jnp.zeros((384, 128), F32)
    for t in range(5):
        col = t * 128 + lane if t < 4 else 512 + (lane & 31)
        atom = jnp.floor((col.astype(F32) + 0.5) * (1.0 / 17.0))
        pick = (col.astype(F32) - 17.0 * atom) == sub.astype(F32)
        src = t * 128 + sub128 if t < 4 else 512 + (sub128 & 31)
        off = src - 17 * lane128
        place = jnp.where(jnp.logical_and(off >= 0, off < 17), 1.0, 0.0).astype(F32)
        for k in range(4):
            for o in range(4):
                if t < 4:
                    line = D[0, k, pl.ds(o * 4 + t, 1), :]
                else:
                    line = jnp.sum(D[1, k, pl.ds(o * 4, 4), :], axis=0, keepdims=True)
                L[pl.ds((o * 4 + k) * 24, 24), :] = jnp.where(pick, line, 0.0)
        total = total + jnp.dot(L[...], place, precision=HIGH, preferred_element_type=F32)
    for k in range(4):
        joined = jnp.zeros((24, 128), F32)
        for o in range(4):
            piece = total[(o * 4 + k) * 24:(o * 4 + k + 1) * 24]
            if o:
                piece = pltpu.roll(piece, o * 32, 1)
            joined = joined + jnp.where((lane >> 5) == o, piece, 0.0)
        N[k] = joined
    pairs = ((0, 0), (0, 1), (0, 2), (1, 1), (1, 2), (2, 2))
    for k in range(4):
        for t, (i, j) in enumerate(pairs):
            W[k * 6 + t, pl.ds(0, 17), :] = (bd[i] * bd[j]) * N[k, pl.ds(0, 17), :]

    def dense_rows(r, carry):
        start = pl.multiple_of(r * 16, 16)
        b = lax.broadcasted_iota(jnp.int32, (16, 128), 0) + r * 16
        for half in range(4):
            acc = [jnp.zeros((16, 128), F32) for _ in range(6)]
            for n in range(17):
                hit = nb[pl.ds(n, 1), :] == b
                for t in range(6):
                    acc[t] = acc[t] + jnp.where(hit, W[half * 6 + t, pl.ds(n, 1), :], 0.0)
            for t, (i, j) in enumerate(pairs):
                block = acc[t].astype(BF)
                DT[half, pl.ds(j * 128 + start, 16), pl.ds(i * 128, 128)] = block
                if i != j:
                    DT[half, pl.ds(i * 128 + start, 16), pl.ds(j * 128, 128)] = block
        return carry

    lax.fori_loop(0, 8, dense_rows, 0)

    def dot(a, b):
        return jnp.dot(a, b, preferred_element_type=F32)

    def dot_t(a, b):
        return lax.dot_general(a, b, (((1,), (1,)), ((), ())), preferred_element_type=F32)

    def mode(m, carry):
        rr, ri = ret[m, 0], ret[m, 1]
        dr, di = DT[2 * m], DT[2 * m + 1]
        HT[0] = (dot(rr, dr) + dot(ri, di)).astype(BF)
        HT[1] = (dot(rr, di) - dot(ri, dr)).astype(BF)
        hr, hi = HT[0], HT[1]
        out[m, 0] = (dot_t(rr, hr) - dot_t(ri, hi)).astype(BF)
        out[m, 1] = (dot_t(rr, hi) + dot_t(ri, hr)).astype(BF)
        return carry

    lax.fori_loop(0, 2, mode, 0)


def phonons(pg, bd, nb, eo, mo, ret):
    vmem = pl.BlockSpec(memory_space=pltpu.VMEM)
    smem = pl.BlockSpec(memory_space=pltpu.SMEM)
    return pl.pallas_call(
        phonon_kernel,
        out_shape=jax.ShapeDtypeStruct((2, 2, 384, 384), BF),
        in_specs=[vmem, vmem, vmem, smem, smem, vmem],
        out_specs=vmem,
        scratch_shapes=[
            pltpu.VMEM((2, 4, 16, 128), F32),
            pltpu.VMEM((384, 128), F32),
            pltpu.VMEM((4, 24, 128), F32),
            pltpu.VMEM((24, 24, 128), F32),
            pltpu.VMEM((4, 384, 384), BF),
            pltpu.VMEM((2, 384, 384), BF),
        ],
        compiler_params=pltpu.CompilerParams(vmem_limit_bytes=40 << 20),
        name="phonon_update",
    )(pg, bd, nb, eo, mo, ret)


def packed_rest(g):
    rest = g[:, 0, :, :, 512:].reshape(2, 2, 4, 4, 9, 32)
    rest = rest.transpose(2, 0, 1, 4, 3, 5).reshape(4, 2, 2, 9, 128)
    return jnp.pad(rest, ((0, 0), (0, 0), (0, 0), (0, 7), (0, 0)))


def local(
    g_less, g_great, d_less, d_ret, neighbours, bond_dirs, energy_offset, momentum_offset, absorb
):
    scale = float(128 * 2 * ORB * ORB) ** (-0.5)
    gl, gg, w = gather(
        g_less, g_great, packed_rest(g_less), packed_rest(g_great), d_less, bond_dirs,
        energy_offset, momentum_offset, absorb,
    )
    main, rest, pg = blocks(
        scale, gl.reshape(2, 16, 2, ROWS, 128), gg.reshape(8, 2, ROWS, 128), w
    )
    d_next = phonons(pg, bond_dirs, neighbours, energy_offset, momentum_offset, d_ret)
    rest = rest[:, :, :, :9].reshape(4, 2, 2, 9, 4, 32).transpose(1, 2, 0, 4, 3, 5)
    rest = rest.reshape(2, 2, 144, 32)
    self_energy = jnp.concatenate([main, rest], axis=3)[:, None]
    return (self_energy, d_next)


def solution(mesh):
    split = Mesh(
        mesh.devices.reshape(4, 4, 4, mesh.shape["momentum"], mesh.shape["phonon"]),
        (X, Y, Z, C, H),
    )
    return jax.shard_map(
        local,
        mesh=split,
        in_specs=(
            P(ENERGY, C, None, None, H),
            P(ENERGY, C, None, None, H),
            P((X, Y, Z, C, H), None, None, None, None),
            P((X, Y, Z, C, H), None, None, None),
            P(), P(), P(), P(), P(),
        ),
        out_specs=(
            P(ENERGY, C, None, None, H),
            P((X, Y, Z, C, H), None, None, None),
        ),
        check_vma=False,
    )
```

```python
import functools

import jax
import jax.numpy as jnp
from jax import lax
from jax.experimental import pallas as pl
from jax.experimental.pallas import tpu as pltpu
from jax.sharding import Mesh
from jax.sharding import PartitionSpec as P

ORB = 12
REACH = 4
X, Y, Z, C, H = ("energy_0", "energy_1", "energy_2", "momentum", "phonon")
ENERGY = (X, Y, Z)
HIGH = lax.Precision.HIGHEST
MESH = pl.DeviceIdType.MESH
ROWS = 160
BF = jnp.bfloat16
F32 = jnp.float32
DMA = pltpu.SemaphoreType.DMA


def others(axis, size):
    here = lax.axis_index(axis)
    return [lax.rem(here + d, size) for d in range(1, size)]


def greet(barrier, **target):
    pl.semaphore_signal(barrier, inc=1, device_id=target, device_id_type=MESH)


def remote(src, dst, send, recv, target):
    return pltpu.make_async_remote_copy(
        src_ref=src, dst_ref=dst, send_sem=send, recv_sem=recv,
        device_id=target, device_id_type=MESH,
    )


def swap(src, dst, send, recv, axis, size):
    here = lax.axis_index(axis)
    copies = []
    for d in range(1, size):
        copies.append(
            remote(src, dst.at[d - 1], send.at[d - 1], recv.at[d - 1],
                   {axis: lax.rem(here + d, size)})
        )
    for c in copies:
        c.start()
    return copies


def whole_kernel(
    scale, gl, gg, rl, rg, dl, bd, nb, eo, mo, ab, ret_in,
    s_out, r_out, d_out,
    GL, GG, CP, YB, YR, T, TC, T0, T1, T2, TY, TX, U, UZ, WQ, WB,
    SB, PA, PS, PC, P0, P2, PXY, PG, PF, D, L, N, W, DT, HT, RET, DO,
    zs_send, zs_recv, gs_send, gs_recv, row_send, row_recv, part_send, part_recv,
    y_send, y_recv, ts_send, ts_recv, ty_send, ty_recv, tx_send, tx_recv, tz_send, tz_recv,
    ta_send, ta_recv, s_send, s_recv, c_send, c_recv, xy_send, xy_recv, pz_send, pz_recv,
    pa_send, pa_recv, io_sem,
):
    x, y, z, c, h = (lax.axis_index(n) for n in (X, Y, Z, C, H))
    row = x * 4 + y
    line = h * 4 + z
    mate = {C: 1 - c}

    barrier = pltpu.get_barrier_semaphore()
    greet(barrier, **mate)
    for d in range(1, 16):
        o = lax.rem(row + d, 16)
        greet(barrier, **{X: o // 4, Y: lax.rem(o, 4)})
        o = lax.rem(line + d, 16)
        greet(barrier, **{Z: lax.rem(o, 4), H: o // 4})

    def own(src, extra, dst, block, sem):
        return [
            pltpu.make_async_copy(
                src.at[:, 0, :, :, pl.ds(pl.multiple_of(z * 128, 128), 128)],
                dst.at[pl.ds(2 * block, 2), :, pl.ds(0, 144), :], sem.at[z, 0]),
            pltpu.make_async_copy(
                extra.at[z], dst.at[pl.ds(2 * block, 2), :, pl.ds(144, 16), :], sem.at[z, 1]),
        ]

    for cp in own(gl, rl, GL.at[0], 2 + z, zs_recv) + own(gg, rg, GG, z, gs_recv):
        cp.start()
    ret_copy = pltpu.make_async_copy(ret_in, RET, io_sem.at[0])
    ret_copy.start()

    lane = lax.broadcasted_iota(jnp.int32, (24, 128), 1)
    CP[...] = jnp.zeros_like(CP)
    for m in range(2):
        for part in range(2):
            total = None
            for i in range(3):
                for j in range(3):
                    term = dl[m, part, 3 * i + j] * (bd[i] * bd[j])
                    total = term if total is None else total + term
            CP[2 * m + part, pl.ds(0, 17), :] = total
    for p in range(4):
        grouped = jnp.zeros((24, 128), F32)
        for k in range(4):
            shift = ((k - p) * 32) % 128
            piece = CP[k]
            if shift:
                piece = pltpu.roll(piece, shift, 1)
            grouped = jnp.where((lane >> 5) == k, piece, grouped)
        YB[p] = grouped
    YR[3] = YB[h]
    PA[...] = jnp.zeros_like(PA)

    @pl.when(row == 0)
    def _():
        GL[:, pl.ds(0, 4)] = jnp.zeros((2, 4, 2, ROWS, 128), BF)

    @pl.when(row == 15)
    def _():
        GL[:, pl.ds(12, 4)] = jnp.zeros((2, 4, 2, ROWS, 128), BF)

    pl.semaphore_wait(barrier, 31)

    y_copies = []
    for d in range(1, 4):
        to = lax.rem(h + d, 4)
        y_copies.append(
            remote(YB.at[to], YR.at[d - 1], y_send.at[d - 1], y_recv.at[d - 1], {H: to})
        )
    for cp in y_copies:
        cp.start()

    def tiles(src, extra, dst, block, send, recv, p):
        return [
            remote(src.at[:, 0, :, :, pl.ds(pl.multiple_of(p * 128, 128), 128)],
                   dst.at[pl.ds(2 * block, 2), :, pl.ds(0, 144), :],
                   send.at[p, 0], recv.at[z, 0], {Z: p}),
            remote(extra.at[p], dst.at[pl.ds(2 * block, 2), :, pl.ds(144, 16), :],
                   send.at[p, 1], recv.at[z, 1], {Z: p}),
        ]

    def less_tiles(p):
        return tiles(gl, rl, GL.at[0], 2 + z, zs_send, zs_recv, p)

    def great_tiles(p):
        return tiles(gg, rg, GG, z, gs_send, gs_recv, p)

    for make in (less_tiles, great_tiles):
        for j in range(4):
            p = jnp.where(z < 2, 3 - j, j)

            @pl.when(p != z)
            def _(make=make, p=p):
                for cp in make(p):
                    cp.start()

    def arrived(dst, block, recv, s):
        for k, (a, n) in enumerate(((0, 144), (144, 16))):
            ref = dst.at[pl.ds(2 * block, 2), :, pl.ds(a, n), :]
            pltpu.make_async_copy(ref, ref, recv.at[s, k]).wait()

    def pair(q, b):
        return GL.at[q, pl.ds(2 * b, 2)]

    def to_mate(b):
        return remote(pair(0, b), pair(1, b), part_send.at[b], part_recv.at[b], mate)

    def next_row(s):
        up = row + 1
        return remote(pair(0, 2 + s), pair(0, s - 2), row_send.at[s], row_recv.at[s],
                      {X: up // 4, Y: lax.rem(up, 4)})

    def last_row(s):
        down = row - 1
        return remote(pair(0, 2 + s), pair(0, s + 6), row_send.at[s], row_recv.at[s],
                      {X: down // 4, Y: lax.rem(down, 4)})

    def forward(s):
        arrived(GL.at[0], 2 + s, zs_recv, s)

        @pl.when(jnp.logical_and(s >= 2, row < 15))
        def _():
            next_row(s).start()

        @pl.when(jnp.logical_and(s < 2, row > 0))
        def _():
            last_row(s).start()

        to_mate(2 + s).start()

    forward(z)

    for cp in y_copies:
        cp.wait_recv()
    lane64 = lane < 64
    base = ((((row * 4 + z) * 2 + c) * 4) * 2)
    label, soak = [], []
    for d in range(4):
        from_h = lax.rem(h + 4 - (d + 1), 4)
        for m in range(2):
            g = base + from_h * 2 + m
            label.append((eo[g] - 1) * 2 + mo[g])
            soak.append(ab[g])
    for q in range(2):
        for e in range(4):
            emit = jnp.zeros((24, 128), F32)
            taken = jnp.zeros((24, 128), F32)
            for d in range(4):
                v = YR[d]
                on = [jnp.where(label[2 * d + m] == 2 * e + q, 1.0, 0.0).astype(F32) for m in range(2)]
                on_s = [on[m] * soak[2 * d + m] for m in range(2)]
                emit = emit + v * jnp.where(lane64, on[0], on[1])
                taken = taken + v * jnp.where(lane64, on_s[0], on_s[1])
            emit = emit + pltpu.roll(emit, 64, 1)
            taken = taken + pltpu.roll(taken, 64, 1)
            T[q, e] = jnp.where(lane64, emit, taken)
    ts = remote(T.at[1 - c], TC, ts_send, ts_recv, mate)
    ts.start()

    forward(lax.rem(z + 1, 4))
    ts.wait_recv()
    T0[...] = T[c] + TC[...]
    tx = swap(T0, TX, tx_send, tx_recv, X, 4)
    forward(lax.rem(z + 3, 4))
    for cp in tx:
        cp.wait_recv()
    T1[...] = (T0[...] + TX[0]) + (TX[1] + TX[2])
    ty = swap(T1, TY, ty_send, ty_recv, Y, 4)
    forward(lax.rem(z + 2, 4))

    @pl.when(row > 0)
    def _():
        for b in (0, 1):
            ref = pair(0, b)
            pltpu.make_async_copy(ref, ref, row_recv.at[b + 2]).wait()
            to_mate(b).start()

    @pl.when(row < 15)
    def _():
        for b in (6, 7):
            ref = pair(0, b)
            pltpu.make_async_copy(ref, ref, row_recv.at[b - 6]).wait()
            to_mate(b).start()

    for cp in ty:
        cp.wait_recv()
    T2[...] = (T1[...] + TY[0]) + (TY[1] + TY[2])

    wide = (24, 640)
    col = lax.broadcasted_iota(jnp.int32, (128, 640), 1)
    col = jnp.where(col < 512, col, 512 + (col & 31))
    src = lax.broadcasted_iota(jnp.int32, (128, 640), 0)
    off = col - 17 * (src & 31)
    inside = jnp.logical_and(off >= 0, off < 17)
    col24 = lax.broadcasted_iota(jnp.int32, wide, 1)
    col24 = jnp.where(col24 < 512, col24, 512 + (col24 & 31)).astype(F32)
    atom = jnp.floor((col24 + 0.5) * (1.0 / 17.0))
    pick = (col24 - 17.0 * atom) == lax.broadcasted_iota(jnp.int32, wide, 0).astype(F32)
    flat = T2[...].reshape(96, 128)
    for k in range(4):
        e_k = jnp.where(jnp.logical_and(inside, (src >> 5) == k), 1.0, 0.0).astype(F32)
        spread = jnp.dot(flat, e_k, precision=HIGH, preferred_element_type=F32)
        for e in range(4):
            w = jnp.sum(jnp.where(pick, spread[e * 24:(e + 1) * 24], 0.0), axis=0, keepdims=True)
            for p in range(4):
                U[p, pl.ds(e * 4 + k, 1), pl.ds(0, 128)] = w[:, p * 128:(p + 1) * 128]
                U[p, pl.ds(e * 4 + k, 1), pl.ds(128, 128)] = w[:, 512:]
    tz = []
    for d in range(1, 4):
        p = lax.rem(z + d, 4)
        tz.append(remote(U.at[p], UZ.at[d - 1], tz_send.at[d - 1], tz_recv.at[d - 1], {Z: p}))
    for cp in tz:
        cp.start()

    def from_mate(b):
        ref = pair(1, b)
        pltpu.make_async_copy(ref, ref, part_recv.at[b]).wait()

    for b in range(2, 6):
        from_mate(b)

    @pl.when(row > 0)
    def _():
        from_mate(0)
        from_mate(1)

    @pl.when(row < 15)
    def _():
        from_mate(6)
        from_mate(7)

    def polar(s):
        arrived(GG, s, gs_recv, s)

        def rows_of(i, carry):
            rows = pl.ds(pl.multiple_of(i * 16, 16), 16)
            acc = [jnp.zeros((8, 128), F32) for _ in range(16)]
            for half in range(2):
                energy = 2 * s + half
                hr = GG[energy, 0, rows, :].astype(F32)
                hi = GG[energy, 1, rows, :].astype(F32)
                for q in range(2):
                    for e in range(4):
                        lr = GL[q, 5 + energy + e, 0, rows, :].astype(F32)
                        li = GL[q, 5 + energy + e, 1, rows, :].astype(F32)
                        re = lr * hr + li * hi
                        im = li * hr - lr * hi
                        k = q * 8 + e * 2
                        acc[k] = acc[k] + (re[:8] + re[8:])
                        acc[k + 1] = acc[k + 1] + (im[:8] + im[8:])
            last = i // 9
            for k in range(16):
                PA[last, k] += acc[k]
            return carry

        lax.fori_loop(0, 10, rows_of, 0)

    for d in (0, 1, 3, 2):
        polar(lax.rem(z + d, 4))
    for q in range(2):
        for last in range(2):
            for k in range(8):
                PS[q, pl.ds(last * 8 + k, 1), :] = (
                    jnp.sum(PA[last, q * 8 + k], axis=0, keepdims=True) * scale
                )
    pc = remote(PS.at[1 - c], PC, c_send, c_recv, mate)
    pc.start()
    for cp in tz:
        cp.wait_recv()
    WQ[c] = (U[z] + UZ[0]) + (UZ[1] + UZ[2])
    ta = remote(WQ.at[c], WQ.at[c], ta_send, ta_recv, mate)
    ta.start()
    pc.wait_recv()
    P0[...] = PS[c] + PC[...]
    pxy = []
    for d in range(1, 16):
        o = lax.rem(row + d, 16)
        pxy.append(remote(P0, PXY.at[d - 1], xy_send.at[d - 1], xy_recv.at[d - 1],
                          {X: o // 4, Y: lax.rem(o, 4)}))
    for cp in pxy:
        cp.start()

    ta.wait_recv()
    for q in range(2):
        for r in range(16):
            w = WQ[q, pl.ds(r, 1), :]
            WB[0, q * 16 + r] = jnp.broadcast_to(w[:, :128], (8, 128))
            WB[1, q * 16 + r] = jnp.broadcast_to(w[:, 128:], (8, 128))

    def sigma_rows(i, carry):
        rows = pl.ds(pl.multiple_of(i * 16, 16), 16)
        last = i // 9
        for energy in range(8):
            re = jnp.zeros((2, 8, 128), F32)
            im = jnp.zeros((2, 8, 128), F32)
            for q in range(2):
                for e in range(4):
                    for k, at in ((0, 3 + energy - e), (2, 5 + energy + e)):
                        br = GL[q, at, 0, rows, :].astype(F32).reshape(2, 8, 128)
                        bi = GL[q, at, 1, rows, :].astype(F32).reshape(2, 8, 128)
                        wr = WB[last, (q * 4 + e) * 4 + k][None]
                        wi = WB[last, (q * 4 + e) * 4 + k + 1][None]
                        re = re + (wr * br - wi * bi)
                        im = im + (wr * bi + wi * br)
            SB[energy, 0, rows, :] = re.reshape(16, 128).astype(BF)
            SB[energy, 1, rows, :] = im.reshape(16, 128).astype(BF)
        return carry

    lax.fori_loop(0, 10, sigma_rows, 0)

    for cp in pxy:
        cp.wait_recv()
    summed = P0[...]
    for d in range(15):
        summed = summed + PXY[d]
    P2[...] = summed.astype(BF)
    PG[c, line] = summed.astype(BF)
    pz = []
    for d in range(1, 16):
        o = lax.rem(line + d, 16)
        pz.append(
            remote(P2, PG.at[c, line], pz_send.at[d - 1], pz_recv.at[d - 1],
                   {Z: lax.rem(o, 4), H: o // 4})
        )
    for d in (8, 7, 9, 6, 10, 5, 11, 4, 12, 3, 13, 2, 14, 1, 15):
        pz[d - 1].start()

    def back(p):
        return [
            remote(SB.at[pl.ds(2 * p, 2), :, pl.ds(0, 144), :],
                   s_out.at[:, :, :, pl.ds(pl.multiple_of(z * 128, 128), 128)],
                   s_send.at[p, 0], s_recv.at[z, 0], {Z: p}),
            remote(SB.at[pl.ds(2 * p, 2), :, pl.ds(144, 16), :], r_out.at[z],
                   s_send.at[p, 1], s_recv.at[z, 1], {Z: p}),
        ]

    for j in range(4):
        p = jnp.where(z < 2, 3 - j, j)

        @pl.when(p != z)
        def _(p=p):
            for cp in back(p):
                cp.start()

    pltpu.make_async_copy(
        SB.at[pl.ds(2 * z, 2), :, pl.ds(0, 144), :],
        s_out.at[:, :, :, pl.ds(pl.multiple_of(z * 128, 128), 128)], s_recv.at[z, 0]).start()
    pltpu.make_async_copy(
        SB.at[pl.ds(2 * z, 2), :, pl.ds(144, 16), :], r_out.at[z], s_recv.at[z, 1]).start()

    for d in range(1, 16):
        o = lax.rem(line + 16 - d, 16)
        ref = PG.at[c, o]
        pltpu.make_async_copy(ref, ref, pz_recv.at[d - 1]).wait()
    pa = remote(PG.at[c], PG.at[c], pa_send, pa_recv, mate)
    pa.start()
    pa.wait_recv()
    PF[...] = PG[...].astype(F32)

    base = ((((x * 4 + y) * 4 + z) * 2 + c) * 4 + h) * 2
    for m in range(2):
        e = jnp.maximum(eo[base + m] - 1, 0)
        q = mo[base + m]
        for part in range(2):
            for o in range(16):
                for last in range(2):
                    D[last, 2 * m + part, pl.ds(o, 1), :] = PF[
                        q, o, pl.ds(last * 8 + e * 2 + part, 1), :]
    sub = lax.broadcasted_iota(jnp.int32, (24, 128), 0)
    lane128 = lax.broadcasted_iota(jnp.int32, (128, 128), 1)
    sub128 = lax.broadcasted_iota(jnp.int32, (128, 128), 0)
    total = jnp.zeros((384, 128), F32)
    for t in range(5):
        col = t * 128 + lane if t < 4 else 512 + (lane & 31)
        atom = jnp.floor((col.astype(F32) + 0.5) * (1.0 / 17.0))
        pick = (col.astype(F32) - 17.0 * atom) == sub.astype(F32)
        src = t * 128 + sub128 if t < 4 else 512 + (sub128 & 31)
        off = src - 17 * lane128
        place = jnp.where(jnp.logical_and(off >= 0, off < 17), 1.0, 0.0).astype(F32)
        for k in range(4):
            for o in range(4):
                if t < 4:
                    w = D[0, k, pl.ds(o * 4 + t, 1), :]
                else:
                    w = jnp.sum(D[1, k, pl.ds(o * 4, 4), :], axis=0, keepdims=True)
                L[pl.ds((o * 4 + k) * 24, 24), :] = jnp.where(pick, w, 0.0)
        total = total + jnp.dot(L[...], place, precision=HIGH, preferred_element_type=F32)
    for k in range(4):
        joined = jnp.zeros((24, 128), F32)
        for o in range(4):
            piece = total[(o * 4 + k) * 24:(o * 4 + k + 1) * 24]
            if o:
                piece = pltpu.roll(piece, o * 32, 1)
            joined = joined + jnp.where((lane >> 5) == o, piece, 0.0)
        N[k] = joined
    pairs = ((0, 0), (0, 1), (0, 2), (1, 1), (1, 2), (2, 2))
    for k in range(4):
        for t, (i, j) in enumerate(pairs):
            W[k * 6 + t, pl.ds(0, 17), :] = (bd[i] * bd[j]) * N[k, pl.ds(0, 17), :]

    def dense_rows(r, carry):
        start = pl.multiple_of(r * 16, 16)
        b = lax.broadcasted_iota(jnp.int32, (16, 128), 0) + r * 16
        for half in range(4):
            acc = [jnp.zeros((16, 128), F32) for _ in range(6)]
            for n in range(17):
                hit = nb[pl.ds(n, 1), :] == b
                for t in range(6):
                    acc[t] = acc[t] + jnp.where(hit, W[half * 6 + t, pl.ds(n, 1), :], 0.0)
            for t, (i, j) in enumerate(pairs):
                block = acc[t].astype(BF)
                DT[half, pl.ds(j * 128 + start, 16), pl.ds(i * 128, 128)] = block
                if i != j:
                    DT[half, pl.ds(i * 128 + start, 16), pl.ds(j * 128, 128)] = block
        return carry

    lax.fori_loop(0, 8, dense_rows, 0)

    def dot(a, b):
        return jnp.dot(a, b, preferred_element_type=F32)

    def dot_t(a, b):
        return lax.dot_general(a, b, (((1,), (1,)), ((), ())), preferred_element_type=F32)

    ret_copy.wait()

    def mode(m, carry):
        rr, ri = RET[m, 0], RET[m, 1]
        dr, di = DT[2 * m], DT[2 * m + 1]
        HT[0] = (dot(rr, dr) + dot(ri, di)).astype(BF)
        HT[1] = (dot(rr, di) - dot(ri, dr)).astype(BF)
        hr, hi = HT[0], HT[1]
        DO[m, 0] = (dot_t(rr, hr) - dot_t(ri, hi)).astype(BF)
        DO[m, 1] = (dot_t(rr, hi) + dot_t(ri, hr)).astype(BF)
        return carry

    lax.fori_loop(0, 2, mode, 0)
    d_copy = pltpu.make_async_copy(DO, d_out, io_sem.at[1])
    d_copy.start()

    for s in range(4):
        main = s_out.at[:, :, :, pl.ds(s * 128, 128)]
        pltpu.make_async_copy(main, main, s_recv.at[s, 0]).wait()
        pltpu.make_async_copy(r_out.at[s], r_out.at[s], s_recv.at[s, 1]).wait()

        @pl.when(z != s)
        def _(s=s):
            for cp in less_tiles(s) + great_tiles(s) + back(s):
                cp.wait_send()

        to_mate(2 + s).wait_send()
    for cp in y_copies + ty + tx + tz + pxy + pz + [ts, ta, pc, pa]:
        cp.wait_send()

    @pl.when(row < 15)
    def _():
        for s in (2, 3):
            next_row(s).wait_send()
        for b in (6, 7):
            to_mate(b).wait_send()

    @pl.when(row > 0)
    def _():
        for s in (0, 1):
            last_row(s).wait_send()
        for b in (0, 1):
            to_mate(b).wait_send()

    d_copy.wait()


def whole(scale, gl, gg, rl, rg, dl, bd, nb, eo, mo, ab, ret):
    anyspace = pl.BlockSpec(memory_space=pl.ANY)
    vmem = pl.BlockSpec(memory_space=pltpu.VMEM)
    smem = pl.BlockSpec(memory_space=pltpu.SMEM)
    t = (4, 24, 128)
    p = (16, 128)

    def f(*shape):
        return pltpu.VMEM(shape, F32)

    def b(*shape):
        return pltpu.VMEM(shape, BF)

    return pl.pallas_call(
        functools.partial(whole_kernel, scale),
        out_shape=(
            jax.ShapeDtypeStruct((2, 2, 144, 512), BF),
            jax.ShapeDtypeStruct((4, 2, 2, 16, 128), BF),
            jax.ShapeDtypeStruct((2, 2, 384, 384), BF),
        ),
        in_specs=[anyspace] * 4 + [vmem] * 3 + [smem] * 3 + [anyspace],
        out_specs=(anyspace,) * 3,
        scratch_shapes=[
            b(2, 16, 2, ROWS, 128), b(8, 2, ROWS, 128),
            f(*t), f(*t), f(*t), f(2, *t), f(*t), f(*t), f(*t), f(*t), f(3, *t), f(3, *t),
            f(4, 16, 256), f(3, 16, 256), f(2, 16, 256), f(2, 32, 8, 128),
            b(8, 2, ROWS, 128), f(2, 16, 8, 128), f(2, *p), f(*p), f(*p), b(*p), f(15, *p),
            b(2, 16, *p), f(2, 16, *p),
            f(2, 4, 16, 128), f(384, 128), f(4, 24, 128), f(24, 24, 128),
            b(4, 384, 384), b(2, 384, 384), b(2, 2, 384, 384), b(2, 2, 384, 384),
            DMA((4, 2)), DMA((4, 2)), DMA((4, 2)), DMA((4, 2)), DMA((4,)), DMA((4,)),
            DMA((8,)), DMA((8,)), DMA((3,)), DMA((3,)), DMA, DMA,
            DMA((3,)), DMA((3,)), DMA((3,)), DMA((3,)), DMA((3,)), DMA((3,)), DMA, DMA,
            DMA((4, 2)), DMA((4, 2)), DMA, DMA, DMA((15,)), DMA((15,)), DMA((15,)), DMA((15,)),
            DMA, DMA, DMA((2,)),
        ],
        compiler_params=pltpu.CompilerParams(
            collective_id=1, has_side_effects=True, vmem_limit_bytes=48 << 20
        ),
        name="whole_step",
    )(gl, gg, rl, rg, dl, bd, nb, eo, mo, ab, ret)


def packed_rest(g):
    rest = g[:, 0, :, :, 512:].reshape(2, 2, 4, 4, 9, 32)
    rest = rest.transpose(2, 0, 1, 4, 3, 5).reshape(4, 2, 2, 9, 128)
    return jnp.pad(rest, ((0, 0), (0, 0), (0, 0), (0, 7), (0, 0)))


def local(
    g_less, g_great, d_less, d_ret, neighbours, bond_dirs, energy_offset, momentum_offset, absorb
):
    scale = float(128 * 2 * ORB * ORB) ** (-0.5)
    main, rest, d_next = whole(
        scale, g_less, g_great, packed_rest(g_less), packed_rest(g_great), d_less, bond_dirs,
        neighbours, energy_offset, momentum_offset, absorb, d_ret,
    )
    rest = rest[:, :, :, :9].reshape(4, 2, 2, 9, 4, 32).transpose(1, 2, 0, 4, 3, 5)
    rest = rest.reshape(2, 2, 144, 32)
    self_energy = jnp.concatenate([main, rest], axis=3)[:, None]
    return (self_energy, d_next)


def solution(mesh):
    split = Mesh(
        mesh.devices.reshape(4, 4, 4, mesh.shape["momentum"], mesh.shape["phonon"]),
        (X, Y, Z, C, H),
    )
    return jax.shard_map(
        local,
        mesh=split,
        in_specs=(
            P(ENERGY, C, None, None, H),
            P(ENERGY, C, None, None, H),
            P((X, Y, Z, C, H), None, None, None, None),
            P((X, Y, Z, C, H), None, None, None),
            P(), P(), P(), P(), P(),
        ),
        out_specs=(
            P(ENERGY, C, None, None, H),
            P((X, Y, Z, C, H), None, None, None),
        ),
        check_vma=False,
    )
```

```python
import functools

import jax
import jax.numpy as jnp
from jax import lax
from jax.experimental import pallas as pl
from jax.experimental.pallas import tpu as pltpu
from jax.sharding import Mesh
from jax.sharding import PartitionSpec as P

ORB = 12
REACH = 4
X, Y, Z, C, H = ("energy_0", "energy_1", "energy_2", "momentum", "phonon")
ENERGY = (X, Y, Z)
HIGH = lax.Precision.HIGHEST
MESH = pl.DeviceIdType.MESH
ROWS = 160
BF = jnp.bfloat16
F32 = jnp.float32
DMA = pltpu.SemaphoreType.DMA


def others(axis, size):
    here = lax.axis_index(axis)
    return [lax.rem(here + d, size) for d in range(1, size)]


def greet(barrier, **target):
    pl.semaphore_signal(barrier, inc=1, device_id=target, device_id_type=MESH)


def remote(src, dst, send, recv, target):
    return pltpu.make_async_remote_copy(
        src_ref=src, dst_ref=dst, send_sem=send, recv_sem=recv,
        device_id=target, device_id_type=MESH,
    )


def swap(src, dst, send, recv, axis, size):
    here = lax.axis_index(axis)
    copies = []
    for d in range(1, size):
        copies.append(
            remote(src, dst.at[d - 1], send.at[d - 1], recv.at[d - 1],
                   {axis: lax.rem(here + d, size)})
        )
    for c in copies:
        c.start()
    return copies


def whole_kernel(
    scale, gl, gg, dl_in, bd_in, nb_in, eo_in, mo_in, ab_in, ret_in,
    s_out, d_out,
    GLV, GGV, DLV, BD, nb, eo, mo, ab, RL, RG, SV, RV,
    GL, GG, CP, YB, YR, T, TC, T0, T1, T2, TY, TX, U, UZ, WQ, WB,
    SB, PA, PS, PC, P0, P2, PXY, PG, PF, D, L, N, W, DT, HT, RET, DO,
    zs_send, zs_recv, gs_send, gs_recv, row_send, row_recv, part_send, part_recv,
    y_send, y_recv, ts_send, ts_recv, ty_send, ty_recv, tx_send, tx_recv, tz_send, tz_recv,
    ta_send, ta_recv, s_send, s_recv, c_send, c_recv, xy_send, xy_recv, pz_send, pz_recv,
    pa_send, pa_recv, io_sem, in_sem,
):
    x, y, z, c, h = (lax.axis_index(n) for n in (X, Y, Z, C, H))
    row = x * 4 + y
    line = h * 4 + z
    mate = {C: 1 - c}

    barrier = pltpu.get_barrier_semaphore()
    greet(barrier, **mate)
    for d in range(1, 16):
        o = lax.rem(row + d, 16)
        greet(barrier, **{X: o // 4, Y: lax.rem(o, 4)})
        o = lax.rem(line + d, 16)
        greet(barrier, **{Z: lax.rem(o, 4), H: o // 4})

    arriving = [
        pltpu.make_async_copy(a, b, in_sem.at[k])
        for k, (a, b) in enumerate((
            (dl_in, DLV), (bd_in, BD), (gl, GLV), (gg, GGV),
            (nb_in, nb), (eo_in, eo), (mo_in, mo), (ab_in, ab), (ret_in, RET),
        ))
    ]

    def own(src, dst, block, sem):
        return pltpu.make_async_copy(
            src.at[:, 0, :, :, pl.ds(pl.multiple_of(z * 128, 128), 128)],
            dst.at[pl.ds(2 * block, 2), :, pl.ds(0, 144), :], sem.at[z, 0])

    for cp in arriving[:4] + [own(gl, GL.at[0], 2 + z, zs_recv), own(gg, GG, z, gs_recv)] + arriving[4:]:
        cp.start()

    lane = lax.broadcasted_iota(jnp.int32, (24, 128), 1)
    CP[...] = jnp.zeros_like(CP)
    for cp in arriving[:2]:
        cp.wait()
    bd = [BD[:, i, :] for i in range(3)]
    squares = [[(bd[i] * bd[j])[:, None, :] for j in range(3)] for i in range(3)]
    for m in range(2):
        total = None
        for i in range(3):
            for j in range(3):
                term = DLV[m, 3 * i + j] * squares[min(i, j)][max(i, j)]
                total = term if total is None else total + term
        for part in range(2):
            CP[2 * m + part, pl.ds(0, 17), :] = total[:, part, :]
    for p in range(4):
        grouped = jnp.zeros((24, 128), F32)
        for k in range(4):
            shift = ((k - p) * 32) % 128
            piece = CP[k]
            if shift:
                piece = pltpu.roll(piece, shift, 1)
            grouped = jnp.where((lane >> 5) == k, piece, grouped)
        YB[p] = grouped
    YR[3] = YB[h]
    PA[...] = jnp.zeros_like(PA)

    @pl.when(row == 0)
    def _():
        GL[:, pl.ds(0, 4)] = jnp.zeros((2, 4, 2, ROWS, 128), BF)

    @pl.when(row == 15)
    def _():
        GL[:, pl.ds(12, 4)] = jnp.zeros((2, 4, 2, ROWS, 128), BF)

    for cp in arriving[2:4]:
        cp.wait()
    blank = jnp.zeros((8, 32), F32)
    for whole_ref, rest_ref in ((GLV, RL), (GGV, RG)):
        for e in range(2):
            for part in range(2):
                v = whole_ref[e, 0, part, :, pl.ds(512, 32)].astype(F32)
                v = [v[8 * g:8 * g + 8] for g in range(18)]
                for p in range(4):
                    top = jnp.concatenate(v[4 * p:4 * p + 4], axis=1)
                    low = jnp.concatenate([v[16 + p] if p < 2 else blank] + [blank] * 3, axis=1)
                    rest_ref[p, e, part] = jnp.concatenate([top, low], axis=0).astype(BF)
    GL[0, pl.ds(2 * (2 + z), 2), :, pl.ds(144, 16), :] = RL[z]
    GG[pl.ds(2 * z, 2), :, pl.ds(144, 16), :] = RG[z]

    pl.semaphore_wait(barrier, 31)

    y_copies = []
    for d in range(1, 4):
        to = lax.rem(h + d, 4)
        y_copies.append(
            remote(YB.at[to], YR.at[d - 1], y_send.at[d - 1], y_recv.at[d - 1], {H: to})
        )
    for cp in y_copies:
        cp.start()

    def tiles(src, extra, dst, block, send, recv, p):
        return [
            remote(src.at[:, 0, :, :, pl.ds(pl.multiple_of(p * 128, 128), 128)],
                   dst.at[pl.ds(2 * block, 2), :, pl.ds(0, 144), :],
                   send.at[p, 0], recv.at[z, 0], {Z: p}),
            remote(extra.at[p], dst.at[pl.ds(2 * block, 2), :, pl.ds(144, 16), :],
                   send.at[p, 1], recv.at[z, 1], {Z: p}),
        ]

    def less_tiles(p):
        return tiles(GLV, RL, GL.at[0], 2 + z, zs_send, zs_recv, p)

    def great_tiles(p):
        return tiles(GGV, RG, GG, z, gs_send, gs_recv, p)

    for make in (less_tiles, great_tiles):
        for j in range(4):
            p = jnp.where(z < 2, 3 - j, j)

            @pl.when(p != z)
            def _(make=make, p=p):
                for cp in make(p):
                    cp.start()

    def arrived(dst, block, recv, s, mine):
        for k, (a, n) in enumerate(((0, 144), (144, 16))[:1 if mine else 2]):
            ref = dst.at[pl.ds(2 * block, 2), :, pl.ds(a, n), :]
            pltpu.make_async_copy(ref, ref, recv.at[s, k]).wait()

    def pair(q, b):
        return GL.at[q, pl.ds(2 * b, 2)]

    def to_mate(b):
        return remote(pair(0, b), pair(1, b), part_send.at[b], part_recv.at[b], mate)

    def next_row(s):
        up = row + 1
        return remote(pair(0, 2 + s), pair(0, s - 2), row_send.at[s], row_recv.at[s],
                      {X: up // 4, Y: lax.rem(up, 4)})

    def last_row(s):
        down = row - 1
        return remote(pair(0, 2 + s), pair(0, s + 6), row_send.at[s], row_recv.at[s],
                      {X: down // 4, Y: lax.rem(down, 4)})

    def forward(s, mine=False):
        arrived(GL.at[0], 2 + s, zs_recv, s, mine)

        @pl.when(jnp.logical_and(s >= 2, row < 15))
        def _():
            next_row(s).start()

        @pl.when(jnp.logical_and(s < 2, row > 0))
        def _():
            last_row(s).start()

        to_mate(2 + s).start()

    forward(z, True)
    forward(lax.rem(z + 1, 4))

    for cp in y_copies:
        cp.wait_recv()
    for cp in arriving[4:]:
        cp.wait()
    lane64 = lane < 64
    base = ((((row * 4 + z) * 2 + c) * 4) * 2)
    label, soak = [], []
    for d in range(4):
        from_h = lax.rem(h + 4 - (d + 1), 4)
        for m in range(2):
            g = base + from_h * 2 + m
            label.append((eo[g] - 1) * 2 + mo[g])
            soak.append(ab[g])
    for q in range(2):
        for e in range(4):
            emit = jnp.zeros((24, 128), F32)
            taken = jnp.zeros((24, 128), F32)
            for d in range(4):
                v = YR[d]
                on = [jnp.where(label[2 * d + m] == 2 * e + q, 1.0, 0.0).astype(F32) for m in range(2)]
                on_s = [on[m] * soak[2 * d + m] for m in range(2)]
                emit = emit + v * jnp.where(lane64, on[0], on[1])
                taken = taken + v * jnp.where(lane64, on_s[0], on_s[1])
            emit = emit + pltpu.roll(emit, 64, 1)
            taken = taken + pltpu.roll(taken, 64, 1)
            T[q, e] = jnp.where(lane64, emit, taken)
    ts = remote(T.at[1 - c], TC, ts_send, ts_recv, mate)
    ts.start()

    forward(lax.rem(z + 3, 4))
    ts.wait_recv()
    T0[...] = T[c] + TC[...]
    tx = swap(T0, TX, tx_send, tx_recv, X, 4)
    forward(lax.rem(z + 2, 4))
    for cp in tx:
        cp.wait_recv()
    T1[...] = (T0[...] + TX[0]) + (TX[1] + TX[2])
    ty = swap(T1, TY, ty_send, ty_recv, Y, 4)

    @pl.when(row > 0)
    def _():
        for b in (0, 1):
            ref = pair(0, b)
            pltpu.make_async_copy(ref, ref, row_recv.at[b + 2]).wait()
            to_mate(b).start()

    @pl.when(row < 15)
    def _():
        for b in (6, 7):
            ref = pair(0, b)
            pltpu.make_async_copy(ref, ref, row_recv.at[b - 6]).wait()
            to_mate(b).start()

    for cp in ty:
        cp.wait_recv()
    T2[...] = (T1[...] + TY[0]) + (TY[1] + TY[2])

    wide = (24, 640)
    col = lax.broadcasted_iota(jnp.int32, (128, 640), 1)
    col = jnp.where(col < 512, col, 512 + (col & 31))
    src = lax.broadcasted_iota(jnp.int32, (128, 640), 0)
    off = col - 17 * (src & 31)
    inside = jnp.logical_and(off >= 0, off < 17)
    col24 = lax.broadcasted_iota(jnp.int32, wide, 1)
    col24 = jnp.where(col24 < 512, col24, 512 + (col24 & 31)).astype(F32)
    atom = jnp.floor((col24 + 0.5) * (1.0 / 17.0))
    pick = (col24 - 17.0 * atom) == lax.broadcasted_iota(jnp.int32, wide, 0).astype(F32)
    flat = T2[...].reshape(96, 128)
    for k in range(4):
        e_k = jnp.where(jnp.logical_and(inside, (src >> 5) == k), 1.0, 0.0).astype(F32)
        spread = jnp.dot(flat, e_k, precision=HIGH, preferred_element_type=F32)
        for e in range(4):
            w = jnp.sum(jnp.where(pick, spread[e * 24:(e + 1) * 24], 0.0), axis=0, keepdims=True)
            for p in range(4):
                U[p, pl.ds(e * 4 + k, 1), pl.ds(0, 128)] = w[:, p * 128:(p + 1) * 128]
                U[p, pl.ds(e * 4 + k, 1), pl.ds(128, 128)] = w[:, 512:]
    tz = []
    for d in range(1, 4):
        p = lax.rem(z + d, 4)
        tz.append(remote(U.at[p], UZ.at[d - 1], tz_send.at[d - 1], tz_recv.at[d - 1], {Z: p}))
    for cp in tz:
        cp.start()

    def from_mate(b):
        ref = pair(1, b)
        pltpu.make_async_copy(ref, ref, part_recv.at[b]).wait()

    for b in range(2, 6):
        from_mate(b)

    @pl.when(row > 0)
    def _():
        from_mate(0)
        from_mate(1)

    @pl.when(row < 15)
    def _():
        from_mate(6)
        from_mate(7)

    def polar(s, mine):
        arrived(GG, s, gs_recv, s, mine)

        def rows_of(i, carry):
            rows = pl.ds(pl.multiple_of(i * 16, 16), 16)
            acc = [jnp.zeros((8, 128), F32) for _ in range(16)]
            for half in range(2):
                energy = 2 * s + half
                hr = GG[energy, 0, rows, :].astype(F32)
                hi = GG[energy, 1, rows, :].astype(F32)
                for q in range(2):
                    for e in range(4):
                        lr = GL[q, 5 + energy + e, 0, rows, :].astype(F32)
                        li = GL[q, 5 + energy + e, 1, rows, :].astype(F32)
                        re = lr * hr + li * hi
                        im = li * hr - lr * hi
                        k = q * 8 + e * 2
                        acc[k] = acc[k] + (re[:8] + re[8:])
                        acc[k + 1] = acc[k + 1] + (im[:8] + im[8:])
            last = i // 9
            for k in range(16):
                PA[last, k] += acc[k]
            return carry

        lax.fori_loop(0, 10, rows_of, 0)

    for d in (0, 1, 3, 2):
        polar(lax.rem(z + d, 4), d == 0)
    for q in range(2):
        for last in range(2):
            for k in range(8):
                PS[q, pl.ds(last * 8 + k, 1), :] = (
                    jnp.sum(PA[last, q * 8 + k], axis=0, keepdims=True) * scale
                )
    pc = remote(PS.at[1 - c], PC, c_send, c_recv, mate)
    pc.start()
    pc.wait_recv()
    P0[...] = PS[c] + PC[...]
    pxy = []
    for d in range(1, 16):
        o = lax.rem(row + d, 16)
        pxy.append(remote(P0, PXY.at[d - 1], xy_send.at[d - 1], xy_recv.at[d - 1],
                          {X: o // 4, Y: lax.rem(o, 4)}))
    for cp in pxy:
        cp.start()

    for cp in tz:
        cp.wait_recv()
    WQ[c] = (U[z] + UZ[0]) + (UZ[1] + UZ[2])
    ta = remote(WQ.at[c], WQ.at[c], ta_send, ta_recv, mate)
    ta.start()
    ta.wait_recv()
    for q in range(2):
        for r in range(16):
            w = WQ[q, pl.ds(r, 1), :]
            WB[0, q * 16 + r] = jnp.broadcast_to(w[:, :128], (8, 128))
            WB[1, q * 16 + r] = jnp.broadcast_to(w[:, 128:], (8, 128))

    def sigma_rows(i, carry):
        rows = pl.ds(pl.multiple_of(i * 16, 16), 16)
        last = i // 9
        for energy in range(8):
            re = jnp.zeros((2, 8, 128), F32)
            im = jnp.zeros((2, 8, 128), F32)
            for q in range(2):
                for e in range(4):
                    for k, at in ((0, 3 + energy - e), (2, 5 + energy + e)):
                        br = GL[q, at, 0, rows, :].astype(F32).reshape(2, 8, 128)
                        bi = GL[q, at, 1, rows, :].astype(F32).reshape(2, 8, 128)
                        wr = WB[last, (q * 4 + e) * 4 + k][None]
                        wi = WB[last, (q * 4 + e) * 4 + k + 1][None]
                        re = re + (wr * br - wi * bi)
                        im = im + (wr * bi + wi * br)
            SB[energy, 0, rows, :] = re.reshape(16, 128).astype(BF)
            SB[energy, 1, rows, :] = im.reshape(16, 128).astype(BF)
        return carry

    lax.fori_loop(0, 10, sigma_rows, 0)

    for cp in pxy:
        cp.wait_recv()
    summed = P0[...]
    for d in range(15):
        summed = summed + PXY[d]
    P2[...] = summed.astype(BF)
    PG[c, line] = summed.astype(BF)
    pz = []
    for d in range(1, 16):
        o = lax.rem(line + d, 16)
        pz.append(
            remote(P2, PG.at[c, line], pz_send.at[d - 1], pz_recv.at[d - 1],
                   {Z: lax.rem(o, 4), H: o // 4})
        )
    for d in (8, 7, 9, 6, 10, 5, 11, 4, 12, 3, 13, 2, 14, 1, 15):
        pz[d - 1].start()

    def back(p):
        return [
            remote(SB.at[pl.ds(2 * p, 2), :, pl.ds(0, 144), :],
                   SV.at[:, 0, :, :, pl.ds(pl.multiple_of(z * 128, 128), 128)],
                   s_send.at[p, 0], s_recv.at[z, 0], {Z: p}),
            remote(SB.at[pl.ds(2 * p, 2), :, pl.ds(144, 16), :], RV.at[z],
                   s_send.at[p, 1], s_recv.at[z, 1], {Z: p}),
        ]

    for j in range(4):
        p = jnp.where(z < 2, 3 - j, j)

        @pl.when(p != z)
        def _(p=p):
            for cp in back(p):
                cp.start()

    SV[:, 0, :, :, pl.ds(pl.multiple_of(z * 128, 128), 128)] = SB[pl.ds(2 * z, 2), :, pl.ds(0, 144), :]
    RV[z] = SB[pl.ds(2 * z, 2), :, pl.ds(144, 16), :]

    for d in range(1, 16):
        o = lax.rem(line + 16 - d, 16)
        ref = PG.at[c, o]
        pltpu.make_async_copy(ref, ref, pz_recv.at[d - 1]).wait()
    pa = remote(PG.at[c], PG.at[c], pa_send, pa_recv, mate)
    pa.start()
    pa.wait_recv()
    PF[...] = PG[...].astype(F32)

    base = ((((x * 4 + y) * 4 + z) * 2 + c) * 4 + h) * 2
    for m in range(2):
        e = jnp.maximum(eo[base + m] - 1, 0)
        q = mo[base + m]
        for part in range(2):
            for o in range(16):
                for last in range(2):
                    D[last, 2 * m + part, pl.ds(o, 1), :] = PF[
                        q, o, pl.ds(last * 8 + e * 2 + part, 1), :]
    sub = lax.broadcasted_iota(jnp.int32, (24, 128), 0)
    lane128 = lax.broadcasted_iota(jnp.int32, (128, 128), 1)
    sub128 = lax.broadcasted_iota(jnp.int32, (128, 128), 0)
    total = jnp.zeros((384, 128), F32)
    for t in range(5):
        col = t * 128 + lane if t < 4 else 512 + (lane & 31)
        atom = jnp.floor((col.astype(F32) + 0.5) * (1.0 / 17.0))
        pick = (col.astype(F32) - 17.0 * atom) == sub.astype(F32)
        src = t * 128 + sub128 if t < 4 else 512 + (sub128 & 31)
        off = src - 17 * lane128
        place = jnp.where(jnp.logical_and(off >= 0, off < 17), 1.0, 0.0).astype(F32)
        for k in range(4):
            for o in range(4):
                if t < 4:
                    w = D[0, k, pl.ds(o * 4 + t, 1), :]
                else:
                    w = jnp.sum(D[1, k, pl.ds(o * 4, 4), :], axis=0, keepdims=True)
                L[pl.ds((o * 4 + k) * 24, 24), :] = jnp.where(pick, w, 0.0)
        total = total + jnp.dot(L[...], place, precision=HIGH, preferred_element_type=F32)
    for k in range(4):
        joined = jnp.zeros((24, 128), F32)
        for o in range(4):
            piece = total[(o * 4 + k) * 24:(o * 4 + k + 1) * 24]
            if o:
                piece = pltpu.roll(piece, o * 32, 1)
            joined = joined + jnp.where((lane >> 5) == o, piece, 0.0)
        N[k] = joined
    pairs = ((0, 0), (0, 1), (0, 2), (1, 1), (1, 2), (2, 2))
    for k in range(4):
        for t, (i, j) in enumerate(pairs):
            W[k * 6 + t, pl.ds(0, 17), :] = (bd[i] * bd[j]) * N[k, pl.ds(0, 17), :]

    def dense_rows(r, carry):
        start = pl.multiple_of(r * 16, 16)
        b = lax.broadcasted_iota(jnp.int32, (16, 128), 0) + r * 16
        for half in range(4):
            acc = [jnp.zeros((16, 128), F32) for _ in range(6)]
            for n in range(17):
                hit = nb[pl.ds(n, 1), :] == b
                for t in range(6):
                    acc[t] = acc[t] + jnp.where(hit, W[half * 6 + t, pl.ds(n, 1), :], 0.0)
            for t, (i, j) in enumerate(pairs):
                block = acc[t].astype(BF)
                DT[half, pl.ds(j * 128 + start, 16), pl.ds(i * 128, 128)] = block
                if i != j:
                    DT[half, pl.ds(i * 128 + start, 16), pl.ds(j * 128, 128)] = block
        return carry

    lax.fori_loop(0, 8, dense_rows, 0)

    def dot(a, b):
        return jnp.dot(a, b, preferred_element_type=F32)

    def dot_t(a, b):
        return lax.dot_general(a, b, (((1,), (1,)), ((), ())), preferred_element_type=F32)


    def mode(m, carry):
        rr, ri = RET[m, 0], RET[m, 1]
        dr, di = DT[2 * m], DT[2 * m + 1]
        HT[0] = (dot(rr, dr) + dot(ri, di)).astype(BF)
        HT[1] = (dot(rr, di) - dot(ri, dr)).astype(BF)
        hr, hi = HT[0], HT[1]
        DO[m, 0] = (dot_t(rr, hr) - dot_t(ri, hi)).astype(BF)
        DO[m, 1] = (dot_t(rr, hi) + dot_t(ri, hr)).astype(BF)
        return carry

    lax.fori_loop(0, 2, mode, 0)
    d_copy = pltpu.make_async_copy(DO, d_out, io_sem.at[1])
    d_copy.start()

    for s in range(4):
        @pl.when(z != s)
        def _(s=s):
            main = SV.at[:, 0, :, :, pl.ds(s * 128, 128)]
            pltpu.make_async_copy(main, main, s_recv.at[s, 0]).wait()
            pltpu.make_async_copy(RV.at[s], RV.at[s], s_recv.at[s, 1]).wait()

    for e in range(2):
        for part in range(2):
            v = [RV[p, e, part].astype(F32) for p in range(4)]
            for p in range(4):
                for k in range(2):
                    two = [v[p][:8, 64 * k + 32 * i:64 * k + 32 * i + 32] for i in range(2)]
                    SV[e, 0, part, pl.ds(32 * p + 16 * k, 16), pl.ds(512, 32)] = (
                        jnp.concatenate(two, axis=0).astype(BF))
            two = [v[p][8:, :32] for p in range(2)]
            SV[e, 0, part, pl.ds(128, 16), pl.ds(512, 32)] = jnp.concatenate(two, axis=0).astype(BF)
    s_copy = pltpu.make_async_copy(SV, s_out, io_sem.at[0])
    s_copy.start()
    for s in range(4):
        @pl.when(z != s)
        def _(s=s):
            for cp in less_tiles(s) + great_tiles(s) + back(s):
                cp.wait_send()

        to_mate(2 + s).wait_send()
    for cp in y_copies + ty + tx + tz + pxy + pz + [ts, ta, pc, pa]:
        cp.wait_send()

    @pl.when(row < 15)
    def _():
        for s in (2, 3):
            next_row(s).wait_send()
        for b in (6, 7):
            to_mate(b).wait_send()

    @pl.when(row > 0)
    def _():
        for s in (0, 1):
            last_row(s).wait_send()
        for b in (0, 1):
            to_mate(b).wait_send()

    d_copy.wait()
    s_copy.wait()


def whole(scale, gl, gg, dl, bd, nb, eo, mo, ab, ret):
    anyspace = pl.BlockSpec(memory_space=pl.ANY)
    t = (4, 24, 128)
    p = (16, 128)

    def f(*shape):
        return pltpu.VMEM(shape, F32)

    def b(*shape):
        return pltpu.VMEM(shape, BF)

    return pl.pallas_call(
        functools.partial(whole_kernel, scale),
        out_shape=(
            jax.ShapeDtypeStruct((2, 1, 2, 144, 544), BF),
            jax.ShapeDtypeStruct((2, 2, 384, 384), BF),
        ),
        in_specs=[anyspace] * 9,
        out_specs=(anyspace,) * 2,
        scratch_shapes=[
            b(2, 1, 2, 144, 544), b(2, 1, 2, 144, 544), f(2, 9, 17, 2, 128), f(17, 3, 128),
            pltpu.VMEM((17, 128), jnp.int32), pltpu.SMEM((1024,), jnp.int32),
            pltpu.SMEM((1024,), jnp.int32), pltpu.SMEM((1024,), F32),
            b(4, 2, 2, 16, 128), b(4, 2, 2, 16, 128), b(2, 1, 2, 144, 544), b(4, 2, 2, 16, 128),
            b(2, 16, 2, ROWS, 128), b(8, 2, ROWS, 128),
            f(*t), f(*t), f(*t), f(2, *t), f(*t), f(*t), f(*t), f(*t), f(3, *t), f(3, *t),
            f(4, 16, 256), f(3, 16, 256), f(2, 16, 256), f(2, 32, 8, 128),
            b(8, 2, ROWS, 128), f(2, 16, 8, 128), f(2, *p), f(*p), f(*p), b(*p), f(15, *p),
            b(2, 16, *p), f(2, 16, *p),
            f(2, 4, 16, 128), f(384, 128), f(4, 24, 128), f(24, 24, 128),
            b(4, 384, 384), b(2, 384, 384), b(2, 2, 384, 384), b(2, 2, 384, 384),
            DMA((4, 2)), DMA((4, 2)), DMA((4, 2)), DMA((4, 2)), DMA((4,)), DMA((4,)),
            DMA((8,)), DMA((8,)), DMA((3,)), DMA((3,)), DMA, DMA,
            DMA((3,)), DMA((3,)), DMA((3,)), DMA((3,)), DMA((3,)), DMA((3,)), DMA, DMA,
            DMA((4, 2)), DMA((4, 2)), DMA, DMA, DMA((15,)), DMA((15,)), DMA((15,)), DMA((15,)),
            DMA, DMA, DMA((2,)), DMA((9,)),
        ],
        compiler_params=pltpu.CompilerParams(
            collective_id=1, has_side_effects=True, vmem_limit_bytes=60 << 20
        ),
        name="whole_step",
    )(gl, gg, dl.transpose(0, 2, 3, 1, 4), bd.transpose(1, 0, 2), nb, eo, mo, ab, ret)


def local(
    g_less, g_great, d_less, d_ret, neighbours, bond_dirs, energy_offset, momentum_offset, absorb
):
    scale = float(128 * 2 * ORB * ORB) ** (-0.5)
    self_energy, d_next = whole(
        scale, g_less, g_great, d_less, bond_dirs, neighbours, energy_offset, momentum_offset,
        absorb, d_ret,
    )
    return (self_energy, d_next)


def solution(mesh):
    split = Mesh(
        mesh.devices.reshape(4, 4, 4, mesh.shape["momentum"], mesh.shape["phonon"]),
        (X, Y, Z, C, H),
    )
    return jax.shard_map(
        local,
        mesh=split,
        in_specs=(
            P(ENERGY, C, None, None, H),
            P(ENERGY, C, None, None, H),
            P((X, Y, Z, C, H), None, None, None, None),
            P((X, Y, Z, C, H), None, None, None),
            P(), P(), P(), P(), P(),
        ),
        out_specs=(
            P(ENERGY, C, None, None, H),
            P((X, Y, Z, C, H), None, None, None),
        ),
        check_vma=False,
    )
```

```python
import functools

import jax
import jax.numpy as jnp
from jax import lax
from jax.experimental import pallas as pl
from jax.experimental.pallas import tpu as pltpu
from jax.sharding import Mesh
from jax.sharding import PartitionSpec as P

ORB = 12
REACH = 4
X, Y, Z, C, H = ("energy_0", "energy_1", "energy_2", "momentum", "phonon")
ENERGY = (X, Y, Z)
HIGH = lax.Precision.HIGHEST
MESH = pl.DeviceIdType.MESH
ROWS = 160
BF = jnp.bfloat16
F32 = jnp.float32
DMA = pltpu.SemaphoreType.DMA


def others(axis, size):
    here = lax.axis_index(axis)
    return [lax.rem(here + d, size) for d in range(1, size)]


def greet(barrier, **target):
    pl.semaphore_signal(barrier, inc=1, device_id=target, device_id_type=MESH)


def remote(src, dst, send, recv, target):
    return pltpu.make_async_remote_copy(
        src_ref=src, dst_ref=dst, send_sem=send, recv_sem=recv,
        device_id=target, device_id_type=MESH,
    )


def swap(src, dst, send, recv, axis, size):
    here = lax.axis_index(axis)
    copies = []
    for d in range(1, size):
        copies.append(
            remote(src, dst.at[d - 1], send.at[d - 1], recv.at[d - 1],
                   {axis: lax.rem(here + d, size)})
        )
    for c in copies:
        c.start()
    return copies


def whole_kernel(
    scale, gl, gg, dl_in, bd_in, nb_in, eo_in, mo_in, ab_in, ret_in,
    s_out, d_out,
    GLV, GGV, DLV, BD, nb, eo, mo, ab, RL, RG, SV, RV,
    GL, GG, CP, YB, YR, T, TC, T0, T1, T2, TY, TX, U, UZ, WQ, WB,
    SB, PA, PS, PC, P0, P2, PXY, PG, PF, D, L, N, W, DT, HT, RET, DO,
    zs_send, zs_recv, gs_send, gs_recv, row_send, row_recv, part_send, part_recv,
    y_send, y_recv, ts_send, ts_recv, ty_send, ty_recv, tx_send, tx_recv, tz_send, tz_recv,
    ta_send, ta_recv, s_send, s_recv, c_send, c_recv, xy_send, xy_recv, pz_send, pz_recv,
    pa_send, pa_recv, io_sem, in_sem,
):
    x, y, z, c, h = (lax.axis_index(n) for n in (X, Y, Z, C, H))
    row = x * 4 + y
    line = h * 4 + z
    mate = {C: 1 - c}

    barrier = pltpu.get_barrier_semaphore()
    greet(barrier, **mate)
    for d in range(1, 16):
        o = lax.rem(row + d, 16)
        greet(barrier, **{X: o // 4, Y: lax.rem(o, 4)})
        o = lax.rem(line + d, 16)
        greet(barrier, **{Z: lax.rem(o, 4), H: o // 4})

    arriving = [
        pltpu.make_async_copy(a, b, in_sem.at[k])
        for k, (a, b) in enumerate((
            (dl_in, DLV), (bd_in, BD), (gl, GLV), (gg, GGV),
            (nb_in, nb), (eo_in, eo), (mo_in, mo), (ab_in, ab), (ret_in, RET),
        ))
    ]

    def own(src, dst, block, sem):
        return pltpu.make_async_copy(
            src.at[:, 0, :, :, pl.ds(pl.multiple_of(z * 128, 128), 128)],
            dst.at[pl.ds(2 * block, 2), :, pl.ds(0, 144), :], sem.at[z, 0])

    for cp in arriving[:4] + [own(gl, GL.at[0], 2 + z, zs_recv), own(gg, GG, z, gs_recv)] + arriving[4:]:
        cp.start()

    lane = lax.broadcasted_iota(jnp.int32, (24, 128), 1)
    CP[...] = jnp.zeros_like(CP)
    for cp in arriving[:2]:
        cp.wait()
    bd = [BD[:, i, :] for i in range(3)]
    squares = [[(bd[i] * bd[j])[:, None, :] for j in range(3)] for i in range(3)]
    for m in range(2):
        total = None
        for i in range(3):
            for j in range(3):
                term = DLV[m, 3 * i + j] * squares[min(i, j)][max(i, j)]
                total = term if total is None else total + term
        for part in range(2):
            CP[2 * m + part, pl.ds(0, 17), :] = total[:, part, :]
    for p in range(4):
        grouped = jnp.zeros((24, 128), F32)
        for k in range(4):
            shift = ((k - p) * 32) % 128
            piece = CP[k]
            if shift:
                piece = pltpu.roll(piece, shift, 1)
            grouped = jnp.where((lane >> 5) == k, piece, grouped)
        YB[p] = grouped
    YR[3] = YB[h]
    PA[...] = jnp.zeros_like(PA)

    @pl.when(row == 0)
    def _():
        GL[:, pl.ds(0, 4)] = jnp.zeros((2, 4, 2, ROWS, 128), BF)

    @pl.when(row == 15)
    def _():
        GL[:, pl.ds(12, 4)] = jnp.zeros((2, 4, 2, ROWS, 128), BF)

    pl.semaphore_wait(barrier, 31)

    y_copies = []
    for d in range(1, 4):
        to = lax.rem(h + d, 4)
        y_copies.append(
            remote(YB.at[to], YR.at[d - 1], y_send.at[d - 1], y_recv.at[d - 1], {H: to})
        )
    for cp in y_copies:
        cp.start()

    far = [jnp.where(z < 2, 3, 0), jnp.where(z < 2, 2, 1), jnp.where(z < 2, 1 - z, 5 - z)]

    def main_tile(src, dst, block, send, recv, p):
        return remote(src.at[:, 0, :, :, pl.ds(pl.multiple_of(p * 128, 128), 128)],
                      dst.at[pl.ds(2 * block, 2), :, pl.ds(0, 144), :],
                      send.at[p, 0], recv.at[z, 0], {Z: p})

    def rest_tile(extra, dst, block, send, recv, p):
        return remote(extra.at[p], dst.at[pl.ds(2 * block, 2), :, pl.ds(144, 16), :],
                      send.at[p, 1], recv.at[z, 1], {Z: p})

    def less_main(p):
        return main_tile(GLV, GL.at[0], 2 + z, zs_send, zs_recv, p)

    def less_rest(p):
        return rest_tile(RL, GL.at[0], 2 + z, zs_send, zs_recv, p)

    def great_main(p):
        return main_tile(GGV, GG, z, gs_send, gs_recv, p)

    def great_rest(p):
        return rest_tile(RG, GG, z, gs_send, gs_recv, p)

    def less_tiles(p):
        return [less_main(p), less_rest(p)]

    def great_tiles(p):
        return [great_main(p), great_rest(p)]

    for cp in arriving[2:4]:
        cp.wait()
    for p in far:
        less_main(p).start()

    blank = jnp.zeros((8, 32), F32)
    for whole_ref, rest_ref in ((GLV, RL), (GGV, RG)):
        for e in range(2):
            for part in range(2):
                v = whole_ref[e, 0, part, :, pl.ds(512, 32)].astype(F32)
                v = [v[8 * g:8 * g + 8] for g in range(18)]
                for p in range(4):
                    top = jnp.concatenate(v[4 * p:4 * p + 4], axis=1)
                    low = jnp.concatenate([v[16 + p] if p < 2 else blank] + [blank] * 3, axis=1)
                    rest_ref[p, e, part] = jnp.concatenate([top, low], axis=0).astype(BF)
    GL[0, pl.ds(2 * (2 + z), 2), :, pl.ds(144, 16), :] = RL[z]
    GG[pl.ds(2 * z, 2), :, pl.ds(144, 16), :] = RG[z]

    for p in far:
        less_rest(p).start()

    def beside(p):
        return jnp.logical_or(p == z - 1, p == z + 1)

    for p in far:
        @pl.when(jnp.logical_not(beside(p)))
        def _(p=p):
            for cp in great_tiles(p):
                cp.start()

    def arrived(dst, block, recv, s, mine):
        for k, (a, n) in enumerate(((0, 144), (144, 16))[:1 if mine else 2]):
            ref = dst.at[pl.ds(2 * block, 2), :, pl.ds(a, n), :]
            pltpu.make_async_copy(ref, ref, recv.at[s, k]).wait()

    def pair(q, b):
        return GL.at[q, pl.ds(2 * b, 2)]

    def to_mate(b):
        return remote(pair(0, b), pair(1, b), part_send.at[b], part_recv.at[b], mate)

    def next_row(s):
        up = row + 1
        return remote(pair(0, 2 + s), pair(0, s - 2), row_send.at[s], row_recv.at[s],
                      {X: up // 4, Y: lax.rem(up, 4)})

    def last_row(s):
        down = row - 1
        return remote(pair(0, 2 + s), pair(0, s + 6), row_send.at[s], row_recv.at[s],
                      {X: down // 4, Y: lax.rem(down, 4)})

    def forward(s, mine=False):
        arrived(GL.at[0], 2 + s, zs_recv, s, mine)

        @pl.when(jnp.logical_and(s >= 2, row < 15))
        def _():
            next_row(s).start()

        @pl.when(jnp.logical_and(s < 2, row > 0))
        def _():
            last_row(s).start()

        to_mate(2 + s).start()

    forward(z, True)

    for cp in y_copies:
        cp.wait_recv()
    for cp in arriving[4:]:
        cp.wait()
    lane64 = lane < 64
    base = ((((row * 4 + z) * 2 + c) * 4) * 2)
    label, soak = [], []
    for d in range(4):
        from_h = lax.rem(h + 4 - (d + 1), 4)
        for m in range(2):
            g = base + from_h * 2 + m
            label.append((eo[g] - 1) * 2 + mo[g])
            soak.append(ab[g])
    for q in range(2):
        for e in range(4):
            emit = jnp.zeros((24, 128), F32)
            taken = jnp.zeros((24, 128), F32)
            for d in range(4):
                v = YR[d]
                on = [jnp.where(label[2 * d + m] == 2 * e + q, 1.0, 0.0).astype(F32) for m in range(2)]
                on_s = [on[m] * soak[2 * d + m] for m in range(2)]
                emit = emit + v * jnp.where(lane64, on[0], on[1])
                taken = taken + v * jnp.where(lane64, on_s[0], on_s[1])
            emit = emit + pltpu.roll(emit, 64, 1)
            taken = taken + pltpu.roll(taken, 64, 1)
            T[q, e] = jnp.where(lane64, emit, taken)
    ts = remote(T.at[1 - c], TC, ts_send, ts_recv, mate)
    ts.start()

    ts.wait_recv()
    T0[...] = T[c] + TC[...]
    ty = swap(T0, TY, ty_send, ty_recv, Y, 4)
    for cp in ty:
        cp.wait_recv()
    T1[...] = (T0[...] + TY[0]) + (TY[1] + TY[2])
    tx = swap(T1, TX, tx_send, tx_recv, X, 4)
    for p in far:
        forward(p)

    for cp in tx:
        cp.wait_recv()
    T2[...] = (T1[...] + TX[0]) + (TX[1] + TX[2])

    wide = (24, 640)
    col = lax.broadcasted_iota(jnp.int32, (128, 640), 1)
    col = jnp.where(col < 512, col, 512 + (col & 31))
    src = lax.broadcasted_iota(jnp.int32, (128, 640), 0)
    off = col - 17 * (src & 31)
    inside = jnp.logical_and(off >= 0, off < 17)
    col24 = lax.broadcasted_iota(jnp.int32, wide, 1)
    col24 = jnp.where(col24 < 512, col24, 512 + (col24 & 31)).astype(F32)
    atom = jnp.floor((col24 + 0.5) * (1.0 / 17.0))
    pick = (col24 - 17.0 * atom) == lax.broadcasted_iota(jnp.int32, wide, 0).astype(F32)
    flat = T2[...].reshape(96, 128)
    for k in range(4):
        e_k = jnp.where(jnp.logical_and(inside, (src >> 5) == k), 1.0, 0.0).astype(F32)
        spread = jnp.dot(flat, e_k, precision=HIGH, preferred_element_type=F32)
        for e in range(4):
            w = jnp.sum(jnp.where(pick, spread[e * 24:(e + 1) * 24], 0.0), axis=0, keepdims=True)
            for p in range(4):
                U[p, pl.ds(e * 4 + k, 1), pl.ds(0, 128)] = w[:, p * 128:(p + 1) * 128]
                U[p, pl.ds(e * 4 + k, 1), pl.ds(128, 128)] = w[:, 512:]
    tz = []
    for d in range(1, 4):
        p = lax.rem(z + d, 4)
        tz.append(remote(U.at[p], UZ.at[d - 1], tz_send.at[d - 1], tz_recv.at[d - 1], {Z: p}))
    for cp in tz:
        cp.start()
    for p in far:
        @pl.when(beside(p))
        def _(p=p):
            for cp in great_tiles(p):
                cp.start()

    @pl.when(row > 0)
    def _():
        for b in (0, 1):
            ref = pair(0, b)
            pltpu.make_async_copy(ref, ref, row_recv.at[b + 2]).wait()
            to_mate(b).start()

    @pl.when(row < 15)
    def _():
        for b in (6, 7):
            ref = pair(0, b)
            pltpu.make_async_copy(ref, ref, row_recv.at[b - 6]).wait()
            to_mate(b).start()

    def from_mate(b):
        ref = pair(1, b)
        pltpu.make_async_copy(ref, ref, part_recv.at[b]).wait()

    for b in range(2, 6):
        from_mate(b)

    @pl.when(row > 0)
    def _():
        from_mate(0)
        from_mate(1)

    @pl.when(row < 15)
    def _():
        from_mate(6)
        from_mate(7)

    def polar(s, mine):
        arrived(GG, s, gs_recv, s, mine)

        def rows_of(i, carry):
            rows = pl.ds(pl.multiple_of(i * 16, 16), 16)
            acc = [jnp.zeros((8, 128), F32) for _ in range(16)]
            for half in range(2):
                energy = 2 * s + half
                hr = GG[energy, 0, rows, :].astype(F32)
                hi = GG[energy, 1, rows, :].astype(F32)
                for q in range(2):
                    for e in range(4):
                        lr = GL[q, 5 + energy + e, 0, rows, :].astype(F32)
                        li = GL[q, 5 + energy + e, 1, rows, :].astype(F32)
                        re = lr * hr + li * hi
                        im = li * hr - lr * hi
                        k = q * 8 + e * 2
                        acc[k] = acc[k] + (re[:8] + re[8:])
                        acc[k + 1] = acc[k + 1] + (im[:8] + im[8:])
            last = i // 9
            for k in range(16):
                PA[last, k] += acc[k]
            return carry

        lax.fori_loop(0, 10, rows_of, 0)

    polar(z, True)
    polar(far[0], False)
    polar(far[1], False)

    for cp in tz:
        cp.wait_recv()
    WQ[c] = (U[z] + UZ[0]) + (UZ[1] + UZ[2])
    ta = remote(WQ.at[c], WQ.at[c], ta_send, ta_recv, mate)
    ta.start()
    ta.wait_recv()
    for q in range(2):
        for r in range(16):
            w = WQ[q, pl.ds(r, 1), :]
            WB[0, q * 16 + r] = jnp.broadcast_to(w[:, :128], (8, 128))
            WB[1, q * 16 + r] = jnp.broadcast_to(w[:, 128:], (8, 128))

    def sigma_rows(i, carry):
        rows = pl.ds(pl.multiple_of(i * 16, 16), 16)
        last = i // 9
        for energy in range(8):
            re = jnp.zeros((2, 8, 128), F32)
            im = jnp.zeros((2, 8, 128), F32)
            for q in range(2):
                for e in range(4):
                    for k, at in ((0, 3 + energy - e), (2, 5 + energy + e)):
                        br = GL[q, at, 0, rows, :].astype(F32).reshape(2, 8, 128)
                        bi = GL[q, at, 1, rows, :].astype(F32).reshape(2, 8, 128)
                        wr = WB[last, (q * 4 + e) * 4 + k][None]
                        wi = WB[last, (q * 4 + e) * 4 + k + 1][None]
                        re = re + (wr * br - wi * bi)
                        im = im + (wr * bi + wi * br)
            SB[energy, 0, rows, :] = re.reshape(16, 128).astype(BF)
            SB[energy, 1, rows, :] = im.reshape(16, 128).astype(BF)
        return carry

    def back(p):
        lanes = pl.ds(pl.multiple_of(z * 128, 128), 128)
        return [
            remote(SB.at[pl.ds(2 * p, 2), :, pl.ds(a, n), :], SV.at[:, 0, :, pl.ds(a, n), lanes],
                   s_send.at[p, k], s_recv.at[z, k], {Z: p})
            for k, (a, n) in enumerate(((0, 80), (80, 64)))
        ] + [
            remote(SB.at[pl.ds(2 * p, 2), :, pl.ds(144, 16), :], RV.at[z],
                   s_send.at[p, 2], s_recv.at[z, 2], {Z: p}),
        ]

    lax.fori_loop(0, 5, sigma_rows, 0)
    for p in far:
        back(p)[0].start()

    polar(far[2], False)
    for q in range(2):
        for last in range(2):
            for k in range(8):
                PS[q, pl.ds(last * 8 + k, 1), :] = (
                    jnp.sum(PA[last, q * 8 + k], axis=0, keepdims=True) * scale
                )
    pc = remote(PS.at[1 - c], PC, c_send, c_recv, mate)
    pc.start()
    pc.wait_recv()
    P0[...] = PS[c] + PC[...]
    pxy = []
    for d in range(1, 16):
        o = lax.rem(row + d, 16)
        pxy.append(remote(P0, PXY.at[d - 1], xy_send.at[d - 1], xy_recv.at[d - 1],
                          {X: o // 4, Y: lax.rem(o, 4)}))
    for cp in pxy:
        cp.start()

    lax.fori_loop(5, 10, sigma_rows, 0)
    for cp in pxy:
        cp.wait_recv()
    summed = P0[...]
    for d in range(15):
        summed = summed + PXY[d]
    P2[...] = summed.astype(BF)
    PG[c, line] = summed.astype(BF)
    pz = []
    for d in range(1, 16):
        o = lax.rem(line + d, 16)
        pz.append(
            remote(P2, PG.at[c, line], pz_send.at[d - 1], pz_recv.at[d - 1],
                   {Z: lax.rem(o, 4), H: o // 4})
        )
    for d in (8, 7, 9, 6, 10, 5, 11, 4, 12, 3, 13, 2, 14, 1, 15):
        pz[d - 1].start()

    for p in far:
        for cp in back(p)[1:]:
            cp.start()
    SV[:, 0, :, :, pl.ds(pl.multiple_of(z * 128, 128), 128)] = SB[pl.ds(2 * z, 2), :, pl.ds(0, 144), :]
    RV[z] = SB[pl.ds(2 * z, 2), :, pl.ds(144, 16), :]

    for d in range(1, 16):
        o = lax.rem(line + 16 - d, 16)
        ref = PG.at[c, o]
        pltpu.make_async_copy(ref, ref, pz_recv.at[d - 1]).wait()
    pa = remote(PG.at[c], PG.at[c], pa_send, pa_recv, mate)
    pa.start()
    pa.wait_recv()
    PF[...] = PG[...].astype(F32)

    base = ((((x * 4 + y) * 4 + z) * 2 + c) * 4 + h) * 2
    for m in range(2):
        e = jnp.maximum(eo[base + m] - 1, 0)
        q = mo[base + m]
        for part in range(2):
            for o in range(16):
                for last in range(2):
                    D[last, 2 * m + part, pl.ds(o, 1), :] = PF[
                        q, o, pl.ds(last * 8 + e * 2 + part, 1), :]
    sub = lax.broadcasted_iota(jnp.int32, (24, 128), 0)
    lane128 = lax.broadcasted_iota(jnp.int32, (128, 128), 1)
    sub128 = lax.broadcasted_iota(jnp.int32, (128, 128), 0)
    total = jnp.zeros((384, 128), F32)
    for t in range(5):
        col = t * 128 + lane if t < 4 else 512 + (lane & 31)
        atom = jnp.floor((col.astype(F32) + 0.5) * (1.0 / 17.0))
        pick = (col.astype(F32) - 17.0 * atom) == sub.astype(F32)
        src = t * 128 + sub128 if t < 4 else 512 + (sub128 & 31)
        off = src - 17 * lane128
        place = jnp.where(jnp.logical_and(off >= 0, off < 17), 1.0, 0.0).astype(F32)
        for k in range(4):
            for o in range(4):
                if t < 4:
                    w = D[0, k, pl.ds(o * 4 + t, 1), :]
                else:
                    w = jnp.sum(D[1, k, pl.ds(o * 4, 4), :], axis=0, keepdims=True)
                L[pl.ds((o * 4 + k) * 24, 24), :] = jnp.where(pick, w, 0.0)
        total = total + jnp.dot(L[...], place, precision=HIGH, preferred_element_type=F32)
    for k in range(4):
        joined = jnp.zeros((24, 128), F32)
        for o in range(4):
            piece = total[(o * 4 + k) * 24:(o * 4 + k + 1) * 24]
            if o:
                piece = pltpu.roll(piece, o * 32, 1)
            joined = joined + jnp.where((lane >> 5) == o, piece, 0.0)
        N[k] = joined
    pairs = ((0, 0), (0, 1), (0, 2), (1, 1), (1, 2), (2, 2))
    for k in range(4):
        for t, (i, j) in enumerate(pairs):
            W[k * 6 + t, pl.ds(0, 17), :] = (bd[i] * bd[j]) * N[k, pl.ds(0, 17), :]

    def dense_rows(r, carry):
        start = pl.multiple_of(r * 16, 16)
        b = lax.broadcasted_iota(jnp.int32, (16, 128), 0) + r * 16
        for half in range(4):
            acc = [jnp.zeros((16, 128), F32) for _ in range(6)]
            for n in range(17):
                hit = nb[pl.ds(n, 1), :] == b
                for t in range(6):
                    acc[t] = acc[t] + jnp.where(hit, W[half * 6 + t, pl.ds(n, 1), :], 0.0)
            for t, (i, j) in enumerate(pairs):
                block = acc[t].astype(BF)
                DT[half, pl.ds(j * 128 + start, 16), pl.ds(i * 128, 128)] = block
                if i != j:
                    DT[half, pl.ds(i * 128 + start, 16), pl.ds(j * 128, 128)] = block
        return carry

    lax.fori_loop(0, 8, dense_rows, 0)

    def dot(a, b):
        return jnp.dot(a, b, preferred_element_type=F32)

    def dot_t(a, b):
        return lax.dot_general(a, b, (((1,), (1,)), ((), ())), preferred_element_type=F32)


    def mode(m, carry):
        rr, ri = RET[m, 0], RET[m, 1]
        dr, di = DT[2 * m], DT[2 * m + 1]
        HT[0] = (dot(rr, dr) + dot(ri, di)).astype(BF)
        HT[1] = (dot(rr, di) - dot(ri, dr)).astype(BF)
        hr, hi = HT[0], HT[1]
        DO[m, 0] = (dot_t(rr, hr) - dot_t(ri, hi)).astype(BF)
        DO[m, 1] = (dot_t(rr, hi) + dot_t(ri, hr)).astype(BF)
        return carry

    lax.fori_loop(0, 2, mode, 0)
    d_copy = pltpu.make_async_copy(DO, d_out, io_sem.at[1])
    d_copy.start()

    for s in range(4):
        @pl.when(z != s)
        def _(s=s):
            for k, (a, n) in enumerate(((0, 80), (80, 64))):
                main = SV.at[:, 0, :, pl.ds(a, n), pl.ds(s * 128, 128)]
                pltpu.make_async_copy(main, main, s_recv.at[s, k]).wait()
            pltpu.make_async_copy(RV.at[s], RV.at[s], s_recv.at[s, 2]).wait()

    for e in range(2):
        for part in range(2):
            v = [RV[p, e, part].astype(F32) for p in range(4)]
            for p in range(4):
                for k in range(2):
                    two = [v[p][:8, 64 * k + 32 * i:64 * k + 32 * i + 32] for i in range(2)]
                    SV[e, 0, part, pl.ds(32 * p + 16 * k, 16), pl.ds(512, 32)] = (
                        jnp.concatenate(two, axis=0).astype(BF))
            two = [v[p][8:, :32] for p in range(2)]
            SV[e, 0, part, pl.ds(128, 16), pl.ds(512, 32)] = jnp.concatenate(two, axis=0).astype(BF)
    s_copy = pltpu.make_async_copy(SV, s_out, io_sem.at[0])
    s_copy.start()
    for s in range(4):
        @pl.when(z != s)
        def _(s=s):
            for cp in less_tiles(s) + great_tiles(s) + back(s):
                cp.wait_send()

        to_mate(2 + s).wait_send()
    for cp in y_copies + ty + tx + tz + pxy + pz + [ts, ta, pc, pa]:
        cp.wait_send()

    @pl.when(row < 15)
    def _():
        for s in (2, 3):
            next_row(s).wait_send()
        for b in (6, 7):
            to_mate(b).wait_send()

    @pl.when(row > 0)
    def _():
        for s in (0, 1):
            last_row(s).wait_send()
        for b in (0, 1):
            to_mate(b).wait_send()

    d_copy.wait()
    s_copy.wait()


def whole(scale, gl, gg, dl, bd, nb, eo, mo, ab, ret):
    anyspace = pl.BlockSpec(memory_space=pl.ANY)
    t = (4, 24, 128)
    p = (16, 128)

    def f(*shape):
        return pltpu.VMEM(shape, F32)

    def b(*shape):
        return pltpu.VMEM(shape, BF)

    return pl.pallas_call(
        functools.partial(whole_kernel, scale),
        out_shape=(
            jax.ShapeDtypeStruct((2, 1, 2, 144, 544), BF),
            jax.ShapeDtypeStruct((2, 2, 384, 384), BF),
        ),
        in_specs=[anyspace] * 9,
        out_specs=(anyspace,) * 2,
        scratch_shapes=[
            b(2, 1, 2, 144, 544), b(2, 1, 2, 144, 544), f(2, 9, 17, 2, 128), f(17, 3, 128),
            pltpu.VMEM((17, 128), jnp.int32), pltpu.SMEM((1024,), jnp.int32),
            pltpu.SMEM((1024,), jnp.int32), pltpu.SMEM((1024,), F32),
            b(4, 2, 2, 16, 128), b(4, 2, 2, 16, 128), b(2, 1, 2, 144, 544), b(4, 2, 2, 16, 128),
            b(2, 16, 2, ROWS, 128), b(8, 2, ROWS, 128),
            f(*t), f(*t), f(*t), f(2, *t), f(*t), f(*t), f(*t), f(*t), f(3, *t), f(3, *t),
            f(4, 16, 256), f(3, 16, 256), f(2, 16, 256), f(2, 32, 8, 128),
            b(8, 2, ROWS, 128), f(2, 16, 8, 128), f(2, *p), f(*p), f(*p), b(*p), f(15, *p),
            b(2, 16, *p), f(2, 16, *p),
            f(2, 4, 16, 128), f(384, 128), f(4, 24, 128), f(24, 24, 128),
            b(4, 384, 384), b(2, 384, 384), b(2, 2, 384, 384), b(2, 2, 384, 384),
            DMA((4, 2)), DMA((4, 2)), DMA((4, 2)), DMA((4, 2)), DMA((4,)), DMA((4,)),
            DMA((8,)), DMA((8,)), DMA((3,)), DMA((3,)), DMA, DMA,
            DMA((3,)), DMA((3,)), DMA((3,)), DMA((3,)), DMA((3,)), DMA((3,)), DMA, DMA,
            DMA((4, 3)), DMA((4, 3)), DMA, DMA, DMA((15,)), DMA((15,)), DMA((15,)), DMA((15,)),
            DMA, DMA, DMA((2,)), DMA((9,)),
        ],
        compiler_params=pltpu.CompilerParams(
            collective_id=1, has_side_effects=True, vmem_limit_bytes=60 << 20
        ),
        name="whole_step",
    )(gl, gg, dl.transpose(0, 2, 3, 1, 4), bd.transpose(1, 0, 2), nb, eo, mo, ab, ret)


def local(
    g_less, g_great, d_less, d_ret, neighbours, bond_dirs, energy_offset, momentum_offset, absorb
):
    scale = float(128 * 2 * ORB * ORB) ** (-0.5)
    self_energy, d_next = whole(
        scale, g_less, g_great, d_less, bond_dirs, neighbours, energy_offset, momentum_offset,
        absorb, d_ret,
    )
    return (self_energy, d_next)


def solution(mesh):
    split = Mesh(
        mesh.devices.reshape(4, 4, 4, mesh.shape["momentum"], mesh.shape["phonon"]),
        (X, Y, Z, C, H),
    )
    return jax.shard_map(
        local,
        mesh=split,
        in_specs=(
            P(ENERGY, C, None, None, H),
            P(ENERGY, C, None, None, H),
            P((X, Y, Z, C, H), None, None, None, None),
            P((X, Y, Z, C, H), None, None, None),
            P(), P(), P(), P(), P(),
        ),
        out_specs=(
            P(ENERGY, C, None, None, H),
            P((X, Y, Z, C, H), None, None, None),
        ),
        check_vma=False,
    )
```

```python
import functools

import jax
import jax.numpy as jnp
from jax import lax
from jax.experimental import pallas as pl
from jax.experimental.pallas import tpu as pltpu
from jax.sharding import Mesh
from jax.sharding import PartitionSpec as P

ORB = 12
REACH = 4
X, Y, Z, C, H = ("energy_0", "energy_1", "energy_2", "momentum", "phonon")
ENERGY = (X, Y, Z)
HIGH = lax.Precision.HIGHEST
MESH = pl.DeviceIdType.MESH
ROWS = 160
BF = jnp.bfloat16
F32 = jnp.float32
DMA = pltpu.SemaphoreType.DMA


def others(axis, size):
    here = lax.axis_index(axis)
    return [lax.rem(here + d, size) for d in range(1, size)]


def greet(barrier, **target):
    pl.semaphore_signal(barrier, inc=1, device_id=target, device_id_type=MESH)


def remote(src, dst, send, recv, target):
    return pltpu.make_async_remote_copy(
        src_ref=src, dst_ref=dst, send_sem=send, recv_sem=recv,
        device_id=target, device_id_type=MESH,
    )


def swap(src, dst, send, recv, axis, size):
    here = lax.axis_index(axis)
    copies = []
    for d in range(1, size):
        copies.append(
            remote(src, dst.at[d - 1], send.at[d - 1], recv.at[d - 1],
                   {axis: lax.rem(here + d, size)})
        )
    for c in copies:
        c.start()
    return copies


def whole_kernel(
    scale, gl, gg, dl_in, bd_in, nb_in, eo_in, mo_in, ab_in, ret_in,
    s_out, d_out,
    GLV, GGV, DLV, BD, nb, eo, mo, ab, RL, RG, SV, RV,
    GL, GG, CP, YB, YR, T, TC, T0, T1, T2, TY, TX, U, UZ, WQ, WB,
    SB, PA, PS, PC, P0, P2, PXY, PG, PF, D, L, N, W, DT, HT, RET, DO,
    zs_send, zs_recv, gs_send, gs_recv, row_send, row_recv, part_send, part_recv,
    y_send, y_recv, ts_send, ts_recv, ty_send, ty_recv, tx_send, tx_recv, tz_send, tz_recv,
    ta_send, ta_recv, s_send, s_recv, c_send, c_recv, xy_send, xy_recv, pz_send, pz_recv,
    pa_send, pa_recv, io_sem, in_sem,
):
    x, y, z, c, h = (lax.axis_index(n) for n in (X, Y, Z, C, H))
    row = x * 4 + y
    line = h * 4 + z
    mate = {C: 1 - c}

    barrier = pltpu.get_barrier_semaphore()
    greet(barrier, **mate)
    for d in range(1, 16):
        o = lax.rem(row + d, 16)
        greet(barrier, **{X: o // 4, Y: lax.rem(o, 4)})
        o = lax.rem(line + d, 16)
        greet(barrier, **{Z: lax.rem(o, 4), H: o // 4})

    arriving = [
        pltpu.make_async_copy(a, b, in_sem.at[k])
        for k, (a, b) in enumerate((
            (dl_in, DLV), (bd_in, BD), (gl, GLV), (gg, GGV),
            (nb_in, nb), (eo_in, eo), (mo_in, mo), (ab_in, ab), (ret_in, RET),
        ))
    ]

    def own(src, dst, block, sem):
        return pltpu.make_async_copy(
            src.at[:, 0, :, :, pl.ds(pl.multiple_of(z * 128, 128), 128)],
            dst.at[pl.ds(2 * block, 2), :, pl.ds(0, 144), :], sem.at[z, 0])

    for cp in arriving[:4] + [own(gl, GL.at[0], 2 + z, zs_recv), own(gg, GG, z, gs_recv)] + arriving[4:]:
        cp.start()

    lane = lax.broadcasted_iota(jnp.int32, (24, 128), 1)
    CP[...] = jnp.zeros_like(CP)
    for cp in arriving[:2]:
        cp.wait()
    bd = [BD[:, i, :] for i in range(3)]
    squares = [[(bd[i] * bd[j])[:, None, :] for j in range(3)] for i in range(3)]
    for m in range(2):
        total = None
        for i in range(3):
            for j in range(3):
                term = DLV[m, 3 * i + j] * squares[min(i, j)][max(i, j)]
                total = term if total is None else total + term
        for part in range(2):
            CP[2 * m + part, pl.ds(0, 17), :] = total[:, part, :]
    for p in range(4):
        grouped = jnp.zeros((24, 128), F32)
        for k in range(4):
            shift = ((k - p) * 32) % 128
            piece = CP[k]
            if shift:
                piece = pltpu.roll(piece, shift, 1)
            grouped = jnp.where((lane >> 5) == k, piece, grouped)
        YB[p] = grouped.astype(BF)
    YR[3] = YB[h]
    PA[...] = jnp.zeros_like(PA)

    @pl.when(row == 0)
    def _():
        GL[:, pl.ds(0, 4)] = jnp.zeros((2, 4, 2, ROWS, 128), BF)

    @pl.when(row == 15)
    def _():
        GL[:, pl.ds(12, 4)] = jnp.zeros((2, 4, 2, ROWS, 128), BF)

    pl.semaphore_wait(barrier, 31)

    y_copies = []
    for d in range(1, 4):
        to = lax.rem(h + d, 4)
        y_copies.append(
            remote(YB.at[to], YR.at[d - 1], y_send.at[d - 1], y_recv.at[d - 1], {H: to})
        )
    for cp in y_copies:
        cp.start()

    far = [jnp.where(z < 2, 3, 0), jnp.where(z < 2, 2, 1), jnp.where(z < 2, 1 - z, 5 - z)]

    def main_tile(src, dst, block, send, recv, p):
        return remote(src.at[:, 0, :, :, pl.ds(pl.multiple_of(p * 128, 128), 128)],
                      dst.at[pl.ds(2 * block, 2), :, pl.ds(0, 144), :],
                      send.at[p, 0], recv.at[z, 0], {Z: p})

    def rest_tile(extra, dst, block, send, recv, p):
        return remote(extra.at[p], dst.at[pl.ds(2 * block, 2), :, pl.ds(144, 16), :],
                      send.at[p, 1], recv.at[z, 1], {Z: p})

    def less_main(p):
        return main_tile(GLV, GL.at[0], 2 + z, zs_send, zs_recv, p)

    def less_rest(p):
        return rest_tile(RL, GL.at[0], 2 + z, zs_send, zs_recv, p)

    def great_main(p):
        return main_tile(GGV, GG, z, gs_send, gs_recv, p)

    def great_rest(p):
        return rest_tile(RG, GG, z, gs_send, gs_recv, p)

    def less_tiles(p):
        return [less_main(p), less_rest(p)]

    def great_tiles(p):
        return [great_main(p), great_rest(p)]

    for cp in arriving[2:4]:
        cp.wait()
    for p in far:
        less_main(p).start()

    blank = jnp.zeros((8, 32), F32)
    for whole_ref, rest_ref in ((GLV, RL), (GGV, RG)):
        for e in range(2):
            for part in range(2):
                v = whole_ref[e, 0, part, :, pl.ds(512, 32)].astype(F32)
                v = [v[8 * g:8 * g + 8] for g in range(18)]
                for p in range(4):
                    top = jnp.concatenate(v[4 * p:4 * p + 4], axis=1)
                    low = jnp.concatenate([v[16 + p] if p < 2 else blank] + [blank] * 3, axis=1)
                    rest_ref[p, e, part] = jnp.concatenate([top, low], axis=0).astype(BF)
    GL[0, pl.ds(2 * (2 + z), 2), :, pl.ds(144, 16), :] = RL[z]
    GG[pl.ds(2 * z, 2), :, pl.ds(144, 16), :] = RG[z]

    for p in far:
        less_rest(p).start()

    def beside(p):
        return jnp.logical_or(p == z - 1, p == z + 1)

    for p in far:
        @pl.when(jnp.logical_not(beside(p)))
        def _(p=p):
            for cp in great_tiles(p):
                cp.start()

    def arrived(dst, block, recv, s, mine):
        for k, (a, n) in enumerate(((0, 144), (144, 16))[:1 if mine else 2]):
            ref = dst.at[pl.ds(2 * block, 2), :, pl.ds(a, n), :]
            pltpu.make_async_copy(ref, ref, recv.at[s, k]).wait()

    def pair(q, b):
        return GL.at[q, pl.ds(2 * b, 2)]

    def to_mate(b):
        return remote(pair(0, b), pair(1, b), part_send.at[b], part_recv.at[b], mate)

    def next_row(s):
        up = row + 1
        return remote(pair(0, 2 + s), pair(0, s - 2), row_send.at[s], row_recv.at[s],
                      {X: up // 4, Y: lax.rem(up, 4)})

    def last_row(s):
        down = row - 1
        return remote(pair(0, 2 + s), pair(0, s + 6), row_send.at[s], row_recv.at[s],
                      {X: down // 4, Y: lax.rem(down, 4)})

    def forward(s, mine=False):
        arrived(GL.at[0], 2 + s, zs_recv, s, mine)

        @pl.when(jnp.logical_and(s >= 2, row < 15))
        def _():
            next_row(s).start()

        @pl.when(jnp.logical_and(s < 2, row > 0))
        def _():
            last_row(s).start()

        to_mate(2 + s).start()

    forward(z, True)

    for cp in y_copies:
        cp.wait_recv()
    for cp in arriving[4:]:
        cp.wait()
    lane64 = lane < 64
    base = ((((row * 4 + z) * 2 + c) * 4) * 2)
    label, soak = [], []
    for d in range(4):
        from_h = lax.rem(h + 4 - (d + 1), 4)
        for m in range(2):
            g = base + from_h * 2 + m
            label.append((eo[g] - 1) * 2 + mo[g])
            soak.append(ab[g])
    for q in range(2):
        for e in range(4):
            emit = jnp.zeros((24, 128), F32)
            taken = jnp.zeros((24, 128), F32)
            for d in range(4):
                v = YR[d].astype(F32)
                on = [jnp.where(label[2 * d + m] == 2 * e + q, 1.0, 0.0).astype(F32) for m in range(2)]
                on_s = [on[m] * soak[2 * d + m] for m in range(2)]
                emit = emit + v * jnp.where(lane64, on[0], on[1])
                taken = taken + v * jnp.where(lane64, on_s[0], on_s[1])
            emit = emit + pltpu.roll(emit, 64, 1)
            taken = taken + pltpu.roll(taken, 64, 1)
            T[q, e] = jnp.where(lane64, emit, taken)
    ts = remote(T.at[1 - c], TC, ts_send, ts_recv, mate)
    ts.start()

    ts.wait_recv()
    T0[...] = T[c] + TC[...]
    ty = swap(T0, TY, ty_send, ty_recv, Y, 4)
    for cp in ty:
        cp.wait_recv()
    T1[...] = (T0[...] + TY[0]) + (TY[1] + TY[2])
    tx = swap(T1, TX, tx_send, tx_recv, X, 4)
    for p in far:
        forward(p)

    for cp in tx:
        cp.wait_recv()
    T2[...] = (T1[...] + TX[0]) + (TX[1] + TX[2])

    wide = (24, 640)
    col = lax.broadcasted_iota(jnp.int32, (128, 640), 1)
    col = jnp.where(col < 512, col, 512 + (col & 31))
    src = lax.broadcasted_iota(jnp.int32, (128, 640), 0)
    off = col - 17 * (src & 31)
    inside = jnp.logical_and(off >= 0, off < 17)
    col24 = lax.broadcasted_iota(jnp.int32, wide, 1)
    col24 = jnp.where(col24 < 512, col24, 512 + (col24 & 31)).astype(F32)
    atom = jnp.floor((col24 + 0.5) * (1.0 / 17.0))
    pick = (col24 - 17.0 * atom) == lax.broadcasted_iota(jnp.int32, wide, 0).astype(F32)
    flat = T2[...].reshape(96, 128)
    for k in range(4):
        e_k = jnp.where(jnp.logical_and(inside, (src >> 5) == k), 1.0, 0.0).astype(F32)
        spread = jnp.dot(flat, e_k, precision=HIGH, preferred_element_type=F32)
        for e in range(4):
            w = jnp.sum(jnp.where(pick, spread[e * 24:(e + 1) * 24], 0.0), axis=0, keepdims=True)
            for p in range(4):
                U[p, pl.ds(e * 4 + k, 1), pl.ds(0, 128)] = w[:, p * 128:(p + 1) * 128]
                U[p, pl.ds(e * 4 + k, 1), pl.ds(128, 128)] = w[:, 512:]
    tz = []
    for d in range(1, 4):
        p = lax.rem(z + d, 4)
        tz.append(remote(U.at[p], UZ.at[d - 1], tz_send.at[d - 1], tz_recv.at[d - 1], {Z: p}))
    for cp in tz:
        cp.start()
    for p in far:
        @pl.when(beside(p))
        def _(p=p):
            for cp in great_tiles(p):
                cp.start()

    @pl.when(row > 0)
    def _():
        for b in (0, 1):
            ref = pair(0, b)
            pltpu.make_async_copy(ref, ref, row_recv.at[b + 2]).wait()
            to_mate(b).start()

    @pl.when(row < 15)
    def _():
        for b in (6, 7):
            ref = pair(0, b)
            pltpu.make_async_copy(ref, ref, row_recv.at[b - 6]).wait()
            to_mate(b).start()

    def from_mate(b):
        ref = pair(1, b)
        pltpu.make_async_copy(ref, ref, part_recv.at[b]).wait()

    for b in range(2, 6):
        from_mate(b)

    @pl.when(row > 0)
    def _():
        from_mate(0)
        from_mate(1)

    @pl.when(row < 15)
    def _():
        from_mate(6)
        from_mate(7)

    def polar(s, mine):
        arrived(GG, s, gs_recv, s, mine)

        def rows_of(i, carry):
            rows = pl.ds(pl.multiple_of(i * 16, 16), 16)
            acc = [jnp.zeros((8, 128), F32) for _ in range(16)]
            for half in range(2):
                energy = 2 * s + half
                hr = GG[energy, 0, rows, :].astype(F32)
                hi = GG[energy, 1, rows, :].astype(F32)
                for q in range(2):
                    for e in range(4):
                        lr = GL[q, 5 + energy + e, 0, rows, :].astype(F32)
                        li = GL[q, 5 + energy + e, 1, rows, :].astype(F32)
                        re = lr * hr + li * hi
                        im = li * hr - lr * hi
                        k = q * 8 + e * 2
                        acc[k] = acc[k] + (re[:8] + re[8:])
                        acc[k + 1] = acc[k + 1] + (im[:8] + im[8:])
            last = i // 9
            for k in range(16):
                PA[last, k] += acc[k]
            return carry

        lax.fori_loop(0, 10, rows_of, 0)

    polar(z, True)
    polar(far[0], False)
    polar(far[1], False)

    for cp in tz:
        cp.wait_recv()
    WQ[c] = (U[z] + UZ[0]) + (UZ[1] + UZ[2])
    ta = remote(WQ.at[c], WQ.at[c], ta_send, ta_recv, mate)
    ta.start()
    ta.wait_recv()
    for q in range(2):
        for r in range(16):
            w = WQ[q, pl.ds(r, 1), :]
            WB[0, q * 16 + r] = jnp.broadcast_to(w[:, :128], (8, 128))
            WB[1, q * 16 + r] = jnp.broadcast_to(w[:, 128:], (8, 128))

    def sigma_rows(i, carry):
        rows = pl.ds(pl.multiple_of(i * 16, 16), 16)
        last = i // 9
        for energy in range(8):
            re = jnp.zeros((2, 8, 128), F32)
            im = jnp.zeros((2, 8, 128), F32)
            for q in range(2):
                for e in range(4):
                    for k, at in ((0, 3 + energy - e), (2, 5 + energy + e)):
                        br = GL[q, at, 0, rows, :].astype(F32).reshape(2, 8, 128)
                        bi = GL[q, at, 1, rows, :].astype(F32).reshape(2, 8, 128)
                        wr = WB[last, (q * 4 + e) * 4 + k][None]
                        wi = WB[last, (q * 4 + e) * 4 + k + 1][None]
                        re = re + (wr * br - wi * bi)
                        im = im + (wr * bi + wi * br)
            SB[energy, 0, rows, :] = re.reshape(16, 128).astype(BF)
            SB[energy, 1, rows, :] = im.reshape(16, 128).astype(BF)
        return carry

    def back(p):
        lanes = pl.ds(pl.multiple_of(z * 128, 128), 128)
        return [
            remote(SB.at[pl.ds(2 * p, 2), :, pl.ds(a, n), :], SV.at[:, 0, :, pl.ds(a, n), lanes],
                   s_send.at[p, k], s_recv.at[z, k], {Z: p})
            for k, (a, n) in enumerate(((0, 80), (80, 64)))
        ] + [
            remote(SB.at[pl.ds(2 * p, 2), :, pl.ds(144, 16), :], RV.at[z],
                   s_send.at[p, 2], s_recv.at[z, 2], {Z: p}),
        ]

    lax.fori_loop(0, 5, sigma_rows, 0)
    for p in far:
        back(p)[0].start()

    polar(far[2], False)
    for q in range(2):
        for last in range(2):
            for k in range(8):
                PS[q, pl.ds(last * 8 + k, 1), :] = (
                    jnp.sum(PA[last, q * 8 + k], axis=0, keepdims=True) * scale
                )
    pc = remote(PS.at[1 - c], PC, c_send, c_recv, mate)
    pc.start()
    pc.wait_recv()
    P0[...] = PS[c] + PC[...]
    pxy = []
    for d in range(1, 16):
        o = lax.rem(row + d, 16)
        pxy.append(remote(P0, PXY.at[d - 1], xy_send.at[d - 1], xy_recv.at[d - 1],
                          {X: o // 4, Y: lax.rem(o, 4)}))
    for cp in pxy:
        cp.start()

    lax.fori_loop(5, 10, sigma_rows, 0)
    for cp in pxy:
        cp.wait_recv()
    summed = P0[...]
    for d in range(15):
        summed = summed + PXY[d]
    P2[...] = summed.astype(BF)
    PG[c, line] = summed.astype(BF)
    pz = []
    for d in range(1, 16):
        o = lax.rem(line + d, 16)
        pz.append(
            remote(P2, PG.at[c, line], pz_send.at[d - 1], pz_recv.at[d - 1],
                   {Z: lax.rem(o, 4), H: o // 4})
        )
    for d in (8, 7, 9, 6, 10, 5, 11, 4, 12, 3, 13, 2, 14, 1, 15):
        pz[d - 1].start()

    for p in far:
        for cp in back(p)[1:]:
            cp.start()
    SV[:, 0, :, :, pl.ds(pl.multiple_of(z * 128, 128), 128)] = SB[pl.ds(2 * z, 2), :, pl.ds(0, 144), :]
    RV[z] = SB[pl.ds(2 * z, 2), :, pl.ds(144, 16), :]

    for d in range(1, 16):
        o = lax.rem(line + 16 - d, 16)
        ref = PG.at[c, o]
        pltpu.make_async_copy(ref, ref, pz_recv.at[d - 1]).wait()
    pa = remote(PG.at[c], PG.at[c], pa_send, pa_recv, mate)
    pa.start()
    pa.wait_recv()
    PF[...] = PG[...].astype(F32)

    base = ((((x * 4 + y) * 4 + z) * 2 + c) * 4 + h) * 2
    for m in range(2):
        e = jnp.maximum(eo[base + m] - 1, 0)
        q = mo[base + m]
        for part in range(2):
            for o in range(16):
                for last in range(2):
                    D[last, 2 * m + part, pl.ds(o, 1), :] = PF[
                        q, o, pl.ds(last * 8 + e * 2 + part, 1), :]
    sub = lax.broadcasted_iota(jnp.int32, (24, 128), 0)
    lane128 = lax.broadcasted_iota(jnp.int32, (128, 128), 1)
    sub128 = lax.broadcasted_iota(jnp.int32, (128, 128), 0)
    total = jnp.zeros((384, 128), F32)
    for t in range(5):
        col = t * 128 + lane if t < 4 else 512 + (lane & 31)
        atom = jnp.floor((col.astype(F32) + 0.5) * (1.0 / 17.0))
        pick = (col.astype(F32) - 17.0 * atom) == sub.astype(F32)
        src = t * 128 + sub128 if t < 4 else 512 + (sub128 & 31)
        off = src - 17 * lane128
        place = jnp.where(jnp.logical_and(off >= 0, off < 17), 1.0, 0.0).astype(F32)
        for k in range(4):
            for o in range(4):
                if t < 4:
                    w = D[0, k, pl.ds(o * 4 + t, 1), :]
                else:
                    w = jnp.sum(D[1, k, pl.ds(o * 4, 4), :], axis=0, keepdims=True)
                L[pl.ds((o * 4 + k) * 24, 24), :] = jnp.where(pick, w, 0.0)
        if t < 4:
            total = total + jnp.dot(L[...].astype(BF), place.astype(BF), preferred_element_type=F32)
        else:
            total = total + jnp.dot(L[...], place, precision=HIGH, preferred_element_type=F32)
    for k in range(4):
        joined = jnp.zeros((24, 128), F32)
        for o in range(4):
            piece = total[(o * 4 + k) * 24:(o * 4 + k + 1) * 24]
            if o:
                piece = pltpu.roll(piece, o * 32, 1)
            joined = joined + jnp.where((lane >> 5) == o, piece, 0.0)
        N[k] = joined
    pairs = ((0, 0), (0, 1), (0, 2), (1, 1), (1, 2), (2, 2))
    for k in range(4):
        for t, (i, j) in enumerate(pairs):
            W[k * 6 + t, pl.ds(0, 17), :] = (bd[i] * bd[j]) * N[k, pl.ds(0, 17), :]

    def dense_rows(r, carry):
        start = pl.multiple_of(r * 16, 16)
        b = lax.broadcasted_iota(jnp.int32, (16, 128), 0) + r * 16
        for half in range(4):
            acc = [jnp.zeros((16, 128), F32) for _ in range(6)]
            for n in range(17):
                hit = nb[pl.ds(n, 1), :] == b
                for t in range(6):
                    acc[t] = acc[t] + jnp.where(hit, W[half * 6 + t, pl.ds(n, 1), :], 0.0)
            for t, (i, j) in enumerate(pairs):
                block = acc[t].astype(BF)
                DT[half, pl.ds(j * 128 + start, 16), pl.ds(i * 128, 128)] = block
                if i != j:
                    DT[half, pl.ds(i * 128 + start, 16), pl.ds(j * 128, 128)] = block
        return carry

    lax.fori_loop(0, 8, dense_rows, 0)

    def dot(a, b):
        return jnp.dot(a, b, preferred_element_type=F32)

    def dot_t(a, b):
        return lax.dot_general(a, b, (((1,), (1,)), ((), ())), preferred_element_type=F32)


    def mode(m, carry):
        rr, ri = RET[m, 0], RET[m, 1]
        dr, di = DT[2 * m], DT[2 * m + 1]
        HT[0] = (dot(rr, dr) + dot(ri, di)).astype(BF)
        HT[1] = (dot(rr, di) - dot(ri, dr)).astype(BF)
        hr, hi = HT[0], HT[1]
        DO[m, 0] = (dot_t(rr, hr) - dot_t(ri, hi)).astype(BF)
        DO[m, 1] = (dot_t(rr, hi) + dot_t(ri, hr)).astype(BF)
        return carry

    lax.fori_loop(0, 2, mode, 0)
    d_copy = pltpu.make_async_copy(DO, d_out, io_sem.at[1])
    d_copy.start()

    for s in range(4):
        @pl.when(z != s)
        def _(s=s):
            for k, (a, n) in enumerate(((0, 80), (80, 64))):
                main = SV.at[:, 0, :, pl.ds(a, n), pl.ds(s * 128, 128)]
                pltpu.make_async_copy(main, main, s_recv.at[s, k]).wait()
            pltpu.make_async_copy(RV.at[s], RV.at[s], s_recv.at[s, 2]).wait()

    for e in range(2):
        for part in range(2):
            v = [RV[p, e, part].astype(F32) for p in range(4)]
            for p in range(4):
                for k in range(2):
                    two = [v[p][:8, 64 * k + 32 * i:64 * k + 32 * i + 32] for i in range(2)]
                    SV[e, 0, part, pl.ds(32 * p + 16 * k, 16), pl.ds(512, 32)] = (
                        jnp.concatenate(two, axis=0).astype(BF))
            two = [v[p][8:, :32] for p in range(2)]
            SV[e, 0, part, pl.ds(128, 16), pl.ds(512, 32)] = jnp.concatenate(two, axis=0).astype(BF)
    s_copy = pltpu.make_async_copy(SV, s_out, io_sem.at[0])
    s_copy.start()
    for s in range(4):
        @pl.when(z != s)
        def _(s=s):
            for cp in less_tiles(s) + great_tiles(s) + back(s):
                cp.wait_send()

        to_mate(2 + s).wait_send()
    for cp in y_copies + ty + tx + tz + pxy + pz + [ts, ta, pc, pa]:
        cp.wait_send()

    @pl.when(row < 15)
    def _():
        for s in (2, 3):
            next_row(s).wait_send()
        for b in (6, 7):
            to_mate(b).wait_send()

    @pl.when(row > 0)
    def _():
        for s in (0, 1):
            last_row(s).wait_send()
        for b in (0, 1):
            to_mate(b).wait_send()

    d_copy.wait()
    s_copy.wait()


def whole(scale, gl, gg, dl, bd, nb, eo, mo, ab, ret):
    anyspace = pl.BlockSpec(memory_space=pl.ANY)
    t = (4, 24, 128)
    p = (16, 128)

    def f(*shape):
        return pltpu.VMEM(shape, F32)

    def b(*shape):
        return pltpu.VMEM(shape, BF)

    return pl.pallas_call(
        functools.partial(whole_kernel, scale),
        out_shape=(
            jax.ShapeDtypeStruct((2, 1, 2, 144, 544), BF),
            jax.ShapeDtypeStruct((2, 2, 384, 384), BF),
        ),
        in_specs=[anyspace] * 9,
        out_specs=(anyspace,) * 2,
        scratch_shapes=[
            b(2, 1, 2, 144, 544), b(2, 1, 2, 144, 544), f(2, 9, 17, 2, 128), f(17, 3, 128),
            pltpu.VMEM((17, 128), jnp.int32), pltpu.SMEM((1024,), jnp.int32),
            pltpu.SMEM((1024,), jnp.int32), pltpu.SMEM((1024,), F32),
            b(4, 2, 2, 16, 128), b(4, 2, 2, 16, 128), b(2, 1, 2, 144, 544), b(4, 2, 2, 16, 128),
            b(2, 16, 2, ROWS, 128), b(8, 2, ROWS, 128),
            f(*t), b(*t), b(*t), f(2, *t), f(*t), f(*t), f(*t), f(*t), f(3, *t), f(3, *t),
            f(4, 16, 256), f(3, 16, 256), f(2, 16, 256), f(2, 32, 8, 128),
            b(8, 2, ROWS, 128), f(2, 16, 8, 128), f(2, *p), f(*p), f(*p), b(*p), f(15, *p),
            b(2, 16, *p), f(2, 16, *p),
            f(2, 4, 16, 128), f(384, 128), f(4, 24, 128), f(24, 24, 128),
            b(4, 384, 384), b(2, 384, 384), b(2, 2, 384, 384), b(2, 2, 384, 384),
            DMA((4, 2)), DMA((4, 2)), DMA((4, 2)), DMA((4, 2)), DMA((4,)), DMA((4,)),
            DMA((8,)), DMA((8,)), DMA((3,)), DMA((3,)), DMA, DMA,
            DMA((3,)), DMA((3,)), DMA((3,)), DMA((3,)), DMA((3,)), DMA((3,)), DMA, DMA,
            DMA((4, 3)), DMA((4, 3)), DMA, DMA, DMA((15,)), DMA((15,)), DMA((15,)), DMA((15,)),
            DMA, DMA, DMA((2,)), DMA((9,)),
        ],
        compiler_params=pltpu.CompilerParams(
            collective_id=1, has_side_effects=True, vmem_limit_bytes=60 << 20
        ),
        name="whole_step",
    )(gl, gg, dl.transpose(0, 2, 3, 1, 4), bd.transpose(1, 0, 2), nb, eo, mo, ab, ret)


def local(
    g_less, g_great, d_less, d_ret, neighbours, bond_dirs, energy_offset, momentum_offset, absorb
):
    scale = float(128 * 2 * ORB * ORB) ** (-0.5)
    self_energy, d_next = whole(
        scale, g_less, g_great, d_less, bond_dirs, neighbours, energy_offset, momentum_offset,
        absorb, d_ret,
    )
    return (self_energy, d_next)


def solution(mesh):
    split = Mesh(
        mesh.devices.reshape(4, 4, 4, mesh.shape["momentum"], mesh.shape["phonon"]),
        (X, Y, Z, C, H),
    )
    return jax.shard_map(
        local,
        mesh=split,
        in_specs=(
            P(ENERGY, C, None, None, H),
            P(ENERGY, C, None, None, H),
            P((X, Y, Z, C, H), None, None, None, None),
            P((X, Y, Z, C, H), None, None, None),
            P(), P(), P(), P(), P(),
        ),
        out_specs=(
            P(ENERGY, C, None, None, H),
            P((X, Y, Z, C, H), None, None, None),
        ),
        check_vma=False,
    )
```
